256 devices in a mesh: blk: 128 (over z, x, y_lo, core), rep: 2 (over y_hi).
Axes of the slice: x: 4, y: 4 (y_hi: 2, y_lo: 2; y = y_hi * 2 + y_lo), z: 8, core: 2. Of those that a mesh axis runs over, the one named last changes fastest.
Arguments:
- particles: bfloat16 [7168, 2048], P(('blk', 'rep')), may hold values from -0.0029907227 to 0.0029907227
- scores: bfloat16 [7168, 2048], P(('blk', 'rep')), may hold values from -60 to 60, as said below
- spread: float32 [1], replicated, may hold values from 0.00034816 to 0.00069632
Outputs:
- direction: float32 [7168, 2048], P(('blk', 'rep'))
The draws below stay inside these ranges and needn't reach their ends.
Inputs may be any that keep to these rules, and one draw needn't show every extreme that they name: `scores`: scores of the particles' log posterior.
All inputs are finite; a program needn't handle non-finite values.
Results may differ from the reference program's by a relative error of at most 0.0003.
Values may be sent and summed in bfloat16 or wider, within the bound.
No kernel may reach another device: no remote copies, remote signals or barrier semaphores. Data moves between devices by JAX's collectives and lax.ppermute only.
A program may use at most 128 MiB of HBM per device.

```python
import math
import jax
import jax.numpy as jnp
from jax import lax

D = 2048
P_SIZE = 7168


def draw_scores(key, part):
    key_common = jax.random.fold_in(key, 11)
    key_rows = jax.random.fold_in(key, 12)
    key_noise = jax.random.fold_in(key, 13)
    upper = 4.0
    common = jax.random.normal(key_common, (D,), jnp.float32)
    row_scale = jnp.exp(jax.random.uniform(key_rows, (P_SIZE, 1), jnp.float32, 0.0, math.log(upper)))
    noise = jax.random.normal(key_noise, (P_SIZE, D), jnp.float32)
    values = jnp.clip(common[None, :] + row_scale * noise, -60.0, 60.0)
    return values.astype(jnp.bfloat16)


def shard_levels(key, dims, cuts, least, largest):
    loudness, own = 1.0, jax.random.fold_in(key, 6)
    for axis_at, blocks in cuts:
        draws = jnp.exp(jax.random.uniform(jax.random.fold_in(own, axis_at), (blocks,), jnp.float32, least / len(cuts), largest / len(cuts)))
        loudness = loudness * jnp.repeat(draws, dims[axis_at] // blocks).reshape([-1 if axis == axis_at else 1 for axis in range(len(dims))])
    return loudness


def gaussian(rng, extent, deviation, reach, split=(), kind=jnp.bfloat16):
    values = deviation * jax.random.normal(rng, extent, jnp.float32)
    if split:
        values = values * shard_levels(rng, extent, split, -0.22, 0.18)
    return jnp.clip(values, -reach, reach).astype(kind)


def setup_inputs(seed: int = 0) -> dict:
    streams_of = jax.random.split(jax.random.key(seed), 4)
    return {
        "particles": gaussian(streams_of[0], (P_SIZE, D), 0.0005, 0.0029907227, ((0, 256),)),
        "scores": draw_scores(jax.random.fold_in(streams_of[3], 71), 0),
        "spread": jnp.clip(jnp.exp(jax.random.uniform(streams_of[2], (1,), jnp.float32, math.log(0.00034816), math.log(0.00069632))), 0.00034816, 0.00069632),
    }


def reference(particles, scores, spread):
    inverse = 1.0 / spread[0]
    population = particles.shape[0]
    particles_wide = particles.astype(jnp.float32)
    norm_all = jnp.sum(particles_wide * particles_wide, axis=1)
    block_rows = math.gcd(population, 512)

    def one_block(block_index):
        first_row = (block_index * block_rows).astype(jnp.int32)
        block_x = lax.dynamic_slice_in_dim(particles, first_row, block_rows, 0)
        block_wide = block_x.astype(jnp.float32)
        block_norm = jnp.sum(block_wide * block_wide, axis=1)
        cross_dots = lax.dot_general(block_x, particles, (((1,), (1,)), ((), ())), preferred_element_type=jnp.float32)
        squared = jnp.maximum(block_norm[:, None] + norm_all[None, :] - 2.0 * cross_dots, 0.0)
        weights = jnp.exp(-squared * inverse)
        weights_low = weights.astype(jnp.bfloat16)
        drive_sum = jnp.dot(weights_low, scores, preferred_element_type=jnp.float32)
        pull_sum = jnp.dot(weights_low, particles, preferred_element_type=jnp.float32)
        row_total = jnp.sum(weights, axis=1)
        return (drive_sum + (2.0 * inverse) * (block_wide * row_total[:, None] - pull_sum)) / population

    blocks = lax.map(one_block, jnp.arange(population // block_rows, dtype=jnp.int32))
    return blocks.reshape(population, particles.shape[1])
```

```python
import jax
import jax.numpy as jnp
from jax import lax
from jax.experimental import pallas as pl
from jax.experimental.pallas import tpu as pltpu
from jax.sharding import Mesh, PartitionSpec as P

PLANE = ("x", "yh", "yl")
AXES = ("z", "x", "yl", "c", "yh")
POPULATION = 7168
ROWS = 28
PAD = 32
DIM = 2048


def sent_to_all(value, axis):
    count = lax.axis_size(axis)
    return lax.all_to_all(
        jnp.broadcast_to(value[None], (count, *value.shape)), axis, 0, 0, tiled=True
    )


def padded(ref, index):
    rows = ref[index]
    fill = jnp.zeros((PAD - ROWS, rows.shape[1]), rows.dtype)
    return jnp.concatenate([rows, fill], axis=0)


def weights_kernel(spread_ref, t_ref, own_ref, other_ref, k_ref, q_ref, t_all, x_all):
    inverse = 1.0 / spread_ref[0]
    for i in range(8):
        t_all[pl.ds(i * PAD, PAD), :] = padded(t_ref, i)
    for i in range(16):
        x_all[pl.ds(i * PAD, PAD), :] = padded(own_ref, i)
        x_all[pl.ds((16 + i) * PAD, PAD), :] = padded(other_ref, i)
    targets = t_all[...]
    source = x_all[...]
    target_wide = targets.astype(jnp.float32)
    source_wide = source.astype(jnp.float32)
    target_norm = jnp.sum(target_wide * target_wide, axis=1, keepdims=True)
    source_norm = jnp.sum(source_wide * source_wide, axis=1, keepdims=True)
    source_norm = jnp.transpose(jnp.broadcast_to(source_norm, (source_norm.shape[0], 128)))[:1]
    dots = lax.dot_general(
        targets, source, (((1,), (1,)), ((), ())), preferred_element_type=jnp.float32
    )
    squared = jnp.maximum(target_norm + source_norm - 2.0 * dots, 0.0)
    weights = jnp.exp(-squared * inverse)
    column = lax.broadcasted_iota(jnp.int32, weights.shape, 1)
    weights = jnp.where(column % PAD < ROWS, weights, 0.0)
    low = weights.astype(jnp.bfloat16)
    k_ref[...] = low
    row_total = jnp.sum(weights, axis=1, keepdims=True)
    pull = jnp.dot(low, source, preferred_element_type=jnp.float32)
    q_ref[...] = (2.0 * inverse) * (target_wide * row_total - pull)


def kernel_weights(spread, targets, own, other):
    return pl.pallas_call(
        weights_kernel,
        in_specs=[
            pl.BlockSpec(memory_space=pltpu.SMEM),
            pl.BlockSpec(memory_space=pltpu.VMEM),
            pl.BlockSpec(memory_space=pltpu.VMEM),
            pl.BlockSpec(memory_space=pltpu.VMEM),
        ],
        out_specs=[
            pl.BlockSpec(memory_space=pltpu.VMEM),
            pl.BlockSpec(memory_space=pltpu.VMEM),
        ],
        out_shape=[
            jax.ShapeDtypeStruct((8 * PAD, 32 * PAD), jnp.bfloat16),
            jax.ShapeDtypeStruct((8 * PAD, DIM), jnp.float32),
        ],
        scratch_shapes=[
            pltpu.VMEM((8 * PAD, DIM), jnp.bfloat16),
            pltpu.VMEM((32 * PAD, DIM), jnp.bfloat16),
        ],
    )(spread, targets, own, other)


def drive_kernel(k_ref, q_ref, own_ref, other_ref, out_ref, s_all):
    for i in range(16):
        s_all[pl.ds(i * PAD, PAD), :] = padded(own_ref, i)
        s_all[pl.ds((16 + i) * PAD, PAD), :] = padded(other_ref, i)
    drive = jnp.dot(k_ref[...], s_all[...], preferred_element_type=jnp.float32)
    total = (drive + q_ref[...]) / POPULATION
    for i in range(8):
        out_ref[pl.ds(i * ROWS, ROWS), :] = total[i * PAD : i * PAD + ROWS]


def partial_direction(weights, rest, own, other):
    width = 512
    return pl.pallas_call(
        drive_kernel,
        grid=(DIM // width,),
        in_specs=[
            pl.BlockSpec((8 * PAD, 32 * PAD), lambda i: (0, 0)),
            pl.BlockSpec((8 * PAD, width), lambda i: (0, i)),
            pl.BlockSpec((16, ROWS, width), lambda i: (0, 0, i)),
            pl.BlockSpec((16, ROWS, width), lambda i: (0, 0, i)),
        ],
        out_specs=pl.BlockSpec((8 * ROWS, width), lambda i: (0, i)),
        out_shape=jax.ShapeDtypeStruct((8 * ROWS, DIM), jnp.float32),
        scratch_shapes=[pltpu.VMEM((32 * PAD, width), jnp.bfloat16)],
    )(weights, rest, own, other)


def shards(particles, scores, spread):
    swap = [(0, 1), (1, 0)]
    targets = sent_to_all(particles, "z")
    own_x = sent_to_all(particles, PLANE)
    own_s = sent_to_all(scores, PLANE)
    other_x = lax.ppermute(own_x, "c", swap)
    weights, rest = kernel_weights(spread, targets, own_x, other_x)
    other_s = lax.ppermute(own_s, "c", swap)
    partial = partial_direction(weights, rest, own_s, other_s)
    return lax.psum_scatter(partial, "z", scatter_dimension=0, tiled=True)


def solution(mesh):
    fine = Mesh(mesh.devices.reshape(8, 4, 2, 2, 2), AXES)
    return jax.shard_map(
        shards,
        mesh=fine,
        in_specs=(P(AXES, None), P(AXES, None), P()),
        out_specs=P(AXES, None),
        check_vma=False,
    )
```

```python
import jax
import jax.numpy as jnp
from jax import lax
from jax.experimental import pallas as pl
from jax.experimental.pallas import tpu as pltpu
from jax.sharding import Mesh, PartitionSpec as P


PLANE = ("x", "yh", "yl")
AXES = ("z", "x", "yl", "c", "yh")
POPULATION = 7168
ROWS = 28
PAD = 32
DIM = 2048
TARGETS = 8
PIECES = 16
STEP = 8


def sent_to_all(value, axis):
    count = lax.axis_size(axis)
    return lax.all_to_all(
        jnp.broadcast_to(value[None], (count, *value.shape)), axis, 0, 0, tiled=True
    )


def padded(rows):
    fill = jnp.zeros((PAD - ROWS, rows.shape[1]), rows.dtype)
    return jnp.concatenate([rows, fill], axis=0)


def row_norms(rows):
    wide = rows.astype(jnp.float32)
    return jnp.sum(wide * wide, axis=1, keepdims=True)


def prepare_kernel(at_ref, *refs):
    t_refs, (t_all, norm_ref) = refs[:TARGETS], refs[TARGETS:]
    for i in range(TARGETS):
        rows = pl.ds(pl.multiple_of(lax.rem(at_ref[0] + TARGETS - i, TARGETS) * PAD, PAD), PAD)
        piece = padded(t_refs[i][...])
        t_all[rows, :] = piece
        norm_ref[rows, :] = jnp.broadcast_to(row_norms(piece), (PAD, 128))


def prepared(at, targets):
    whole = TARGETS * PAD
    return pl.pallas_call(
        prepare_kernel,
        in_specs=[pl.BlockSpec(memory_space=pltpu.SMEM)]
        + [pl.BlockSpec(memory_space=pltpu.VMEM)] * TARGETS,
        out_specs=[pl.BlockSpec(memory_space=pltpu.VMEM)] * 2,
        out_shape=[
            jax.ShapeDtypeStruct((whole, DIM), jnp.bfloat16),
            jax.ShapeDtypeStruct((whole, 128), jnp.float32),
        ],
    )(at, *targets)


def half_kernel(first, spread_ref, t_all, norm_ref, source_ref, *refs):
    if first:
        out_ref, x_all, s_all = refs
    else:
        before_ref, out_ref, x_all, s_all, total_ref = refs
    step = pl.program_id(0)
    inverse = 1.0 / spread_ref[0]
    for i in range(STEP):
        x_all[pl.ds(i * PAD, PAD), :] = padded(source_ref[i, :ROWS])
        s_all[pl.ds(i * PAD, PAD), :] = padded(source_ref[i, ROWS:])
    targets = t_all[...]
    source = x_all[...]
    source_norm = row_norms(source)
    source_norm = jnp.transpose(jnp.broadcast_to(source_norm, (STEP * PAD, 128)))[:1]
    dots = lax.dot_general(
        targets, source, (((1,), (1,)), ((), ())), preferred_element_type=jnp.float32
    )
    squared = jnp.maximum(norm_ref[:, :1] + source_norm - 2.0 * dots, 0.0)
    weights = jnp.exp(-squared * inverse)
    column = lax.broadcasted_iota(jnp.int32, weights.shape, 1)
    weights = jnp.where(column % PAD < ROWS, weights, 0.0)
    low = weights.astype(jnp.bfloat16)
    row_total = jnp.sum(weights, axis=1, keepdims=True)
    pull = jnp.dot(low, source, preferred_element_type=jnp.float32)
    drive = jnp.dot(low, s_all[...], preferred_element_type=jnp.float32)
    added = drive + (2.0 * inverse) * (targets.astype(jnp.float32) * row_total - pull)
    last = pl.num_programs(0) - 1
    if first:

        @pl.when(step == 0)
        def _():
            out_ref[...] = added

        @pl.when(step > 0)
        def _():
            out_ref[...] += added

    else:

        @pl.when(step == 0)
        def _():
            total_ref[...] = before_ref[...] + added

        @pl.when(step == last)
        def _():
            total = (total_ref[...] + added) / POPULATION
            for i in range(TARGETS):
                out_ref[pl.ds(i * ROWS, ROWS), :] = total[i * PAD : i * PAD + ROWS]


def half(spread, targets, norms, source, before=None):
    first = before is None
    whole = TARGETS * PAD
    rows = whole if first else TARGETS * ROWS
    in_specs = [
        pl.BlockSpec(memory_space=pltpu.SMEM),
        pl.BlockSpec((whole, DIM), lambda i: (0, 0)),
        pl.BlockSpec((whole, 128), lambda i: (0, 0)),
        pl.BlockSpec((STEP, 2 * ROWS, DIM), lambda i: (i, 0, 0)),
    ]
    args = [spread, targets, norms, source]
    scratch = [pltpu.VMEM((STEP * PAD, DIM), jnp.bfloat16)] * 2
    if not first:
        in_specs.append(pl.BlockSpec((whole, DIM), lambda i: (0, 0)))
        args.append(before)
        scratch.append(pltpu.VMEM((whole, DIM), jnp.float32))

    def body(*refs):
        half_kernel(first, *refs)

    return pl.pallas_call(
        body,
        grid=(PIECES // STEP,),
        in_specs=in_specs,
        out_specs=pl.BlockSpec((rows, DIM), lambda i: (0, 0)),
        out_shape=jax.ShapeDtypeStruct((rows, DIM), jnp.float32),
        scratch_shapes=scratch,
        compiler_params=pltpu.CompilerParams(dimension_semantics=("arbitrary",)),
    )(*args)


def direction(particles, scores, spread):
    swap = [(0, 1), (1, 0)]
    at = lax.axis_index("z").astype(jnp.int32)[None]
    pieces = [particles] + [
        lax.ppermute(particles, "z", [(i, (i + k) % TARGETS) for i in range(TARGETS)])
        for k in range(1, TARGETS)
    ]
    targets, norms = prepared(at, pieces)
    own = sent_to_all(jnp.concatenate([particles, scores], axis=0), PLANE)
    other = lax.ppermute(own, "c", swap)
    before = half(spread, targets, norms, own)
    partial = half(spread, targets, norms, other, before)
    return lax.psum_scatter(partial, "z", scatter_dimension=0, tiled=True)


def solution(mesh):
    fine = Mesh(mesh.devices.reshape(8, 4, 2, 2, 2), AXES)
    return jax.shard_map(
        direction,
        mesh=fine,
        in_specs=(P(AXES, None), P(AXES, None), P()),
        out_specs=P(AXES, None),
        check_vma=False,
    )
```

```python
import jax
import jax.numpy as jnp
from jax import lax
from jax.experimental import pallas as pl
from jax.experimental.pallas import tpu as pltpu
from jax.sharding import Mesh, PartitionSpec as P


PLANE = ("x", "yh", "yl")
AXES = ("z", "x", "yl", "c", "yh")
POPULATION = 7168
ROWS = 28
PAD = 32
DIM = 2048
TARGETS = 8
PIECES = 16
STEP = 8


def sent_to_all(value, axis):
    count = lax.axis_size(axis)
    return lax.all_to_all(
        jnp.broadcast_to(value[None], (count, *value.shape)), axis, 0, 0, tiled=True
    )


def padded(rows):
    fill = jnp.zeros((PAD - ROWS, rows.shape[1]), rows.dtype)
    return jnp.concatenate([rows, fill], axis=0)


def row_norms(rows):
    wide = rows.astype(jnp.float32)
    return jnp.sum(wide * wide, axis=1, keepdims=True)


def prepare_kernel(at_ref, own_ref, up_ref, down_ref, far_up_ref, far_down_ref, t_all, norm_ref):
    half = DIM // 2

    def put(offset, ref, index):
        slot = lax.rem(at_ref[0] + TARGETS + offset, TARGETS)
        rows = pl.ds(pl.multiple_of(slot * PAD, PAD), PAD)
        at = index * 2 * ROWS
        left = padded(ref[at : at + ROWS])
        right = padded(ref[at + ROWS : at + 2 * ROWS])
        t_all[rows, :half] = left
        t_all[rows, half:] = right
        norm_ref[rows, :] = jnp.broadcast_to(row_norms(left) + row_norms(right), (PAD, 128))

    put(0, own_ref, 0)
    put(-1, up_ref, 0)
    put(1, down_ref, 0)
    for i, offset in enumerate((-2, -3, -4)):
        put(offset, far_up_ref, i)
    for i, offset in enumerate((2, 3)):
        put(offset, far_down_ref, i)


def prepared(at, pieces):
    whole = TARGETS * PAD
    return pl.pallas_call(
        prepare_kernel,
        in_specs=[pl.BlockSpec(memory_space=pltpu.SMEM)]
        + [pl.BlockSpec(memory_space=pltpu.VMEM)] * len(pieces),
        out_specs=[pl.BlockSpec(memory_space=pltpu.VMEM)] * 2,
        out_shape=[
            jax.ShapeDtypeStruct((whole, DIM), jnp.bfloat16),
            jax.ShapeDtypeStruct((whole, 128), jnp.float32),
        ],
    )(at, *pieces)


def moved(value, steps):
    return lax.ppermute(value, "z", [(i, (i + steps) % TARGETS) for i in range(TARGETS)])


def half_kernel(first, spread_ref, t_all, norm_ref, source_ref, *refs):
    if first:
        out_ref, x_all, s_all = refs
    else:
        before_ref, out_ref, x_all, s_all, total_ref = refs
    step = pl.program_id(0)
    inverse = 1.0 / spread_ref[0]
    for i in range(STEP):
        x_all[pl.ds(i * PAD, PAD), :] = padded(source_ref[i, :ROWS])
        s_all[pl.ds(i * PAD, PAD), :] = padded(source_ref[i, ROWS:])
    targets = t_all[...]
    source = x_all[...]
    source_norm = row_norms(source)
    source_norm = jnp.transpose(jnp.broadcast_to(source_norm, (STEP * PAD, 128)))[:1]
    dots = lax.dot_general(
        targets, source, (((1,), (1,)), ((), ())), preferred_element_type=jnp.float32
    )
    squared = jnp.maximum(norm_ref[:, :1] + source_norm - 2.0 * dots, 0.0)
    weights = jnp.exp(-squared * inverse)
    column = lax.broadcasted_iota(jnp.int32, weights.shape, 1)
    weights = jnp.where(column % PAD < ROWS, weights, 0.0)
    low = weights.astype(jnp.bfloat16)
    row_total = jnp.sum(weights, axis=1, keepdims=True)
    pull = jnp.dot(low, source, preferred_element_type=jnp.float32)
    drive = jnp.dot(low, s_all[...], preferred_element_type=jnp.float32)
    added = drive + (2.0 * inverse) * (targets.astype(jnp.float32) * row_total - pull)
    last = pl.num_programs(0) - 1
    if first:

        @pl.when(step == 0)
        def _():
            out_ref[...] = added

        @pl.when(step > 0)
        def _():
            out_ref[...] += added

    else:

        @pl.when(step == 0)
        def _():
            total_ref[...] = before_ref[...] + added

        @pl.when(step == last)
        def _():
            total = (total_ref[...] + added) / POPULATION
            for i in range(TARGETS):
                out_ref[pl.ds(i * ROWS, ROWS), :] = total[i * PAD : i * PAD + ROWS]


def half(spread, targets, norms, source, before=None):
    first = before is None
    whole = TARGETS * PAD
    rows = whole if first else TARGETS * ROWS
    in_specs = [
        pl.BlockSpec(memory_space=pltpu.SMEM),
        pl.BlockSpec((whole, DIM), lambda i: (0, 0)),
        pl.BlockSpec((whole, 128), lambda i: (0, 0)),
        pl.BlockSpec((STEP, 2 * ROWS, DIM), lambda i: (i, 0, 0)),
    ]
    args = [spread, targets, norms, source]
    scratch = [pltpu.VMEM((STEP * PAD, DIM), jnp.bfloat16)] * 2
    if not first:
        in_specs.append(pl.BlockSpec((whole, DIM), lambda i: (0, 0)))
        args.append(before)
        scratch.append(pltpu.VMEM((whole, DIM), jnp.float32))

    def body(*refs):
        half_kernel(first, *refs)

    return pl.pallas_call(
        body,
        grid=(PIECES // STEP,),
        in_specs=in_specs,
        out_specs=pl.BlockSpec((rows, DIM), lambda i: (0, 0)),
        out_shape=jax.ShapeDtypeStruct((rows, DIM), jnp.float32),
        scratch_shapes=scratch,
        compiler_params=pltpu.CompilerParams(dimension_semantics=("arbitrary",)),
    )(*args)


def direction(particles, scores, spread):
    swap = [(0, 1), (1, 0)]
    at = lax.axis_index("z").astype(jnp.int32)[None]
    own_piece = jnp.concatenate([particles[:, : DIM // 2], particles[:, DIM // 2 :]], axis=0)
    up, down = moved(own_piece, 1), moved(own_piece, -1)
    far_up = moved(jnp.concatenate([down, own_piece, up], axis=0), 3)
    far_down = moved(jnp.concatenate([up, own_piece], axis=0), -3)
    pieces = [own_piece, up, down, far_up, far_down]
    targets, norms = prepared(at, pieces)
    own = sent_to_all(jnp.concatenate([particles, scores], axis=0), PLANE)
    other = lax.ppermute(own, "c", swap)
    before = half(spread, targets, norms, own)
    partial = half(spread, targets, norms, other, before)
    return lax.psum_scatter(partial, "z", scatter_dimension=0, tiled=True)


def solution(mesh):
    fine = Mesh(mesh.devices.reshape(8, 4, 2, 2, 2), AXES)
    return jax.shard_map(
        direction,
        mesh=fine,
        in_specs=(P(AXES, None), P(AXES, None), P()),
        out_specs=P(AXES, None),
        check_vma=False,
    )
```

```python
import jax
import jax.numpy as jnp
from jax import lax
from jax.experimental import pallas as pl
from jax.experimental.pallas import tpu as pltpu
from jax.sharding import Mesh, PartitionSpec as P


PLANE = ("x", "yh", "yl")
AXES = ("z", "x", "yl", "c", "yh")
POPULATION = 7168
ROWS = 28
PAD = 32
SPAN = 31
DIM = 2048
TARGETS = 8
PIECES = 16
STEP = 8


def sent_to_all(value, axis):
    count = lax.axis_size(axis)
    return lax.all_to_all(
        jnp.broadcast_to(value[None], (count, *value.shape)), axis, 0, 0, tiled=True
    )


def padded(rows):
    fill = jnp.zeros((PAD - ROWS, rows.shape[1]), rows.dtype)
    return jnp.concatenate([rows, fill], axis=0)


def row_norms(rows):
    wide = rows.astype(jnp.float32)
    return jnp.sum(wide * wide, axis=1, keepdims=True)


def prepare_kernel(at_ref, own_ref, up_ref, down_ref, far_up_ref, far_down_ref, t_all, norm_ref):
    half = DIM // 2

    def put(offset, ref, index):
        slot = lax.rem(at_ref[0] + TARGETS + offset, TARGETS)
        rows = pl.ds(pl.multiple_of(slot * PAD, PAD), PAD)
        at = index * 2 * ROWS
        left = padded(ref[at : at + ROWS])
        right = padded(ref[at + ROWS : at + 2 * ROWS])
        t_all[rows, :half] = left
        t_all[rows, half:] = right
        norm_ref[rows, :] = jnp.broadcast_to(row_norms(left) + row_norms(right), (PAD, 128))

    put(0, own_ref, 0)
    put(-1, up_ref, 0)
    put(1, down_ref, 0)
    for i, offset in enumerate((-2, -3, -4)):
        put(offset, far_up_ref, i)
    for i, offset in enumerate((2, 3)):
        put(offset, far_down_ref, i)


def prepared(at, pieces):
    whole = TARGETS * PAD
    return pl.pallas_call(
        prepare_kernel,
        in_specs=[pl.BlockSpec(memory_space=pltpu.SMEM)]
        + [pl.BlockSpec(memory_space=pltpu.VMEM)] * len(pieces),
        out_specs=[pl.BlockSpec(memory_space=pltpu.VMEM)] * 2,
        out_shape=[
            jax.ShapeDtypeStruct((whole, DIM), jnp.bfloat16),
            jax.ShapeDtypeStruct((whole, 128), jnp.float32),
        ],
    )(at, *pieces)


def moved(value, steps):
    return lax.ppermute(value, "z", [(i, (i + steps) % TARGETS) for i in range(TARGETS)])


def half_kernel(spread_ref, t_all, norm_ref, source_ref, out_ref, x_all, s_all, total_ref):
    step = pl.program_id(0)
    inverse = 1.0 / spread_ref[0]
    for i in range(STEP):
        x_all[pl.ds(i * PAD, PAD), :] = padded(source_ref[i, :ROWS])
        s_all[pl.ds(i * PAD, PAD), :] = padded(source_ref[i, ROWS:])
    targets = t_all[...]
    source = x_all[...]
    source_norm = row_norms(source)
    source_norm = jnp.transpose(jnp.broadcast_to(source_norm, (STEP * PAD, 128)))[:1]
    dots = lax.dot_general(
        targets, source, (((1,), (1,)), ((), ())), preferred_element_type=jnp.float32
    )
    squared = jnp.maximum(norm_ref[:, :1] + source_norm - 2.0 * dots, 0.0)
    weights = jnp.exp(-squared * inverse)
    column = lax.broadcasted_iota(jnp.int32, weights.shape, 1)
    weights = jnp.where(column % PAD < ROWS, weights, 0.0)
    low = weights.astype(jnp.bfloat16)
    row_total = jnp.sum(weights, axis=1, keepdims=True)
    pull = jnp.dot(low, source, preferred_element_type=jnp.float32)
    drive = jnp.dot(low, s_all[...], preferred_element_type=jnp.float32)
    added = drive + (2.0 * inverse) * (targets.astype(jnp.float32) * row_total - pull)
    last = pl.num_programs(0) - 1

    @pl.when(step == 0)
    def _():
        total_ref[...] = added

    @pl.when(step == last)
    def _():
        total = total_ref[...] + added
        for i in range(TARGETS):
            out_ref[pl.ds(i * SPAN, SPAN), :] = total[i * PAD : i * PAD + SPAN]


def half(spread, targets, norms, source):
    whole = TARGETS * PAD
    return pl.pallas_call(
        half_kernel,
        grid=(PIECES // STEP,),
        in_specs=[
            pl.BlockSpec(memory_space=pltpu.SMEM),
            pl.BlockSpec((whole, DIM), lambda i: (0, 0)),
            pl.BlockSpec((whole, 128), lambda i: (0, 0)),
            pl.BlockSpec((STEP, 2 * ROWS, DIM), lambda i: (i, 0, 0)),
        ],
        out_specs=pl.BlockSpec((TARGETS * SPAN, DIM), lambda i: (0, 0)),
        out_shape=jax.ShapeDtypeStruct((TARGETS * SPAN, DIM), jnp.float32),
        scratch_shapes=[
            pltpu.VMEM((STEP * PAD, DIM), jnp.bfloat16),
            pltpu.VMEM((STEP * PAD, DIM), jnp.bfloat16),
            pltpu.VMEM((whole, DIM), jnp.float32),
        ],
        compiler_params=pltpu.CompilerParams(dimension_semantics=("arbitrary",)),
    )(spread, targets, norms, source)


def direction(particles, scores, spread):
    swap = [(0, 1), (1, 0)]
    at = lax.axis_index("z").astype(jnp.int32)[None]
    own_piece = jnp.concatenate([particles[:, : DIM // 2], particles[:, DIM // 2 :]], axis=0)
    up, down = moved(own_piece, 1), moved(own_piece, -1)
    far_up = moved(jnp.concatenate([down, own_piece, up], axis=0), 3)
    far_down = moved(jnp.concatenate([up, own_piece], axis=0), -3)
    pieces = [own_piece, up, down, far_up, far_down]
    targets, norms = prepared(at, pieces)
    own = sent_to_all(jnp.concatenate([particles, scores], axis=0), PLANE)
    other = lax.ppermute(own, "c", swap)
    mine = half(spread, targets, norms, own)
    theirs = half(spread, targets, norms, other)
    partial = (mine + theirs) / POPULATION
    total = lax.psum_scatter(partial, "z", scatter_dimension=0, tiled=True)
    return lax.optimization_barrier(total)[:ROWS]


def solution(mesh):
    fine = Mesh(mesh.devices.reshape(8, 4, 2, 2, 2), AXES)
    return jax.shard_map(
        direction,
        mesh=fine,
        in_specs=(P(AXES, None), P(AXES, None), P()),
        out_specs=P(AXES, None),
        check_vma=False,
    )
```

```python
import jax
import jax.numpy as jnp
from jax import lax
from jax.experimental import pallas as pl
from jax.experimental.pallas import tpu as pltpu
from jax.sharding import Mesh, PartitionSpec as P


AXES = ("z", "x", "yl", "c", "yh")
POPULATION = 7168
ROWS = 28
PAD = 32
SPAN = 31
DIM = 2048
TARGETS = 8
PIECES = 16
STEP = 8


def device_at(z, x, y, core):
    return (((z * 4 + x) * 2 + y % 2) * 2 + core) * 2 + y // 2


def plane_lines(along_x):
    groups = []
    for z in range(TARGETS):
        for core in range(2):
            for at in range(4):
                if (core == 0) == along_x:
                    groups.append([device_at(z, i, at, core) for i in range(4)])
                else:
                    groups.append([device_at(z, at, i, core) for i in range(4)])
    return groups


def sent_along(value, groups):
    count = len(groups[0])
    arrived = lax.all_to_all(
        jnp.broadcast_to(value[None], (count, *value.shape)),
        AXES,
        0,
        0,
        tiled=True,
        axis_index_groups=groups,
    )
    return arrived.reshape(count * value.shape[0], *value.shape[1:])


def padded(rows):
    fill = jnp.zeros((PAD - ROWS, rows.shape[1]), rows.dtype)
    return jnp.concatenate([rows, fill], axis=0)


def row_norms(rows):
    wide = rows.astype(jnp.float32)
    return jnp.sum(wide * wide, axis=1, keepdims=True)


def prepare_kernel(at_ref, own_ref, up_ref, down_ref, far_up_ref, far_down_ref, t_all, norm_ref):
    half = DIM // 2

    def put(offset, ref, index):
        slot = lax.rem(at_ref[0] + TARGETS + offset, TARGETS)
        rows = pl.ds(pl.multiple_of(slot * PAD, PAD), PAD)
        at = index * 2 * ROWS
        left = padded(ref[at : at + ROWS])
        right = padded(ref[at + ROWS : at + 2 * ROWS])
        t_all[rows, :half] = left
        t_all[rows, half:] = right
        norm_ref[rows, :] = jnp.broadcast_to(row_norms(left) + row_norms(right), (PAD, 128))

    put(0, own_ref, 0)
    put(-1, up_ref, 0)
    put(1, down_ref, 0)
    for i, offset in enumerate((-2, -3, -4)):
        put(offset, far_up_ref, i)
    for i, offset in enumerate((2, 3)):
        put(offset, far_down_ref, i)


def prepared(at, pieces):
    whole = TARGETS * PAD
    return pl.pallas_call(
        prepare_kernel,
        in_specs=[pl.BlockSpec(memory_space=pltpu.SMEM)]
        + [pl.BlockSpec(memory_space=pltpu.VMEM)] * len(pieces),
        out_specs=[pl.BlockSpec(memory_space=pltpu.VMEM)] * 2,
        out_shape=[
            jax.ShapeDtypeStruct((whole, DIM), jnp.bfloat16),
            jax.ShapeDtypeStruct((whole, 128), jnp.float32),
        ],
    )(at, *pieces)


def moved(value, steps):
    return lax.ppermute(value, "z", [(i, (i + steps) % TARGETS) for i in range(TARGETS)])


def half_kernel(spread_ref, t_all, norm_ref, source_ref, out_ref, x_all, s_all, total_ref):
    step = pl.program_id(0)
    inverse = 1.0 / spread_ref[0]
    for i in range(STEP):
        x_all[pl.ds(i * PAD, PAD), :] = padded(source_ref[i, :ROWS])
        s_all[pl.ds(i * PAD, PAD), :] = padded(source_ref[i, ROWS:])
    targets = t_all[...]
    source = x_all[...]
    source_norm = row_norms(source)
    source_norm = jnp.transpose(jnp.broadcast_to(source_norm, (STEP * PAD, 128)))[:1]
    dots = lax.dot_general(
        targets, source, (((1,), (1,)), ((), ())), preferred_element_type=jnp.float32
    )
    squared = jnp.maximum(norm_ref[:, :1] + source_norm - 2.0 * dots, 0.0)
    weights = jnp.exp(-squared * inverse)
    column = lax.broadcasted_iota(jnp.int32, weights.shape, 1)
    weights = jnp.where(column % PAD < ROWS, weights, 0.0)
    low = weights.astype(jnp.bfloat16)
    row_total = jnp.sum(weights, axis=1, keepdims=True)
    pull = jnp.dot(low, source, preferred_element_type=jnp.float32)
    drive = jnp.dot(low, s_all[...], preferred_element_type=jnp.float32)
    added = drive + (2.0 * inverse) * (targets.astype(jnp.float32) * row_total - pull)
    last = pl.num_programs(0) - 1

    @pl.when(step == 0)
    def _():
        total_ref[...] = added

    @pl.when(step == last)
    def _():
        total = total_ref[...] + added
        for i in range(TARGETS):
            out_ref[pl.ds(i * SPAN, SPAN), :] = total[i * PAD : i * PAD + SPAN]


def half(spread, targets, norms, source):
    whole = TARGETS * PAD
    return pl.pallas_call(
        half_kernel,
        grid=(PIECES // STEP,),
        in_specs=[
            pl.BlockSpec(memory_space=pltpu.SMEM),
            pl.BlockSpec((whole, DIM), lambda i: (0, 0)),
            pl.BlockSpec((whole, 128), lambda i: (0, 0)),
            pl.BlockSpec((STEP, 2 * ROWS, DIM), lambda i: (i, 0, 0)),
        ],
        out_specs=pl.BlockSpec((TARGETS * SPAN, DIM), lambda i: (0, 0)),
        out_shape=jax.ShapeDtypeStruct((TARGETS * SPAN, DIM), jnp.float32),
        scratch_shapes=[
            pltpu.VMEM((STEP * PAD, DIM), jnp.bfloat16),
            pltpu.VMEM((STEP * PAD, DIM), jnp.bfloat16),
            pltpu.VMEM((whole, DIM), jnp.float32),
        ],
        compiler_params=pltpu.CompilerParams(dimension_semantics=("arbitrary",)),
    )(spread, targets, norms, source)


def direction(particles, scores, spread):
    swap = [(0, 1), (1, 0)]
    at = lax.axis_index("z").astype(jnp.int32)[None]
    own_piece = jnp.concatenate([particles[:, : DIM // 2], particles[:, DIM // 2 :]], axis=0)
    up, down = moved(own_piece, 1), moved(own_piece, -1)
    far_up = moved(jnp.concatenate([down, own_piece, up], axis=0), 3)
    far_down = moved(jnp.concatenate([up, own_piece], axis=0), -3)
    targets, norms = prepared(at, [own_piece, up, down, far_up, far_down])
    line = sent_along(jnp.concatenate([particles, scores], axis=0), plane_lines(True))
    own = sent_along(line, plane_lines(False)).reshape(PIECES, 2 * ROWS, DIM)
    other = lax.ppermute(own, "c", swap)
    mine = half(spread, targets, norms, own)
    theirs = half(spread, targets, norms, other)
    partial = (mine + theirs) / POPULATION
    total = lax.psum_scatter(partial, "z", scatter_dimension=0, tiled=True)
    return lax.optimization_barrier(total)[:ROWS]


def solution(mesh):
    fine = Mesh(mesh.devices.reshape(8, 4, 2, 2, 2), AXES)
    return jax.shard_map(
        direction,
        mesh=fine,
        in_specs=(P(AXES, None), P(AXES, None), P()),
        out_specs=P(AXES, None),
        check_vma=False,
    )
```

```python
import jax
import jax.numpy as jnp
from jax import lax
from jax.experimental import pallas as pl
from jax.experimental.pallas import tpu as pltpu
from jax.sharding import Mesh, PartitionSpec as P


AXES = ("z", "x", "yl", "c", "yh")
POPULATION = 7168
ROWS = 28
PAD = 32
SPAN = 31
CUT = 32
DIM = 2048
TARGETS = 8
PIECES = 16
STEP = 8
CHUNK = 4
WIDTH = 512


def device_at(z, x, y, core):
    return (((z * 4 + x) * 2 + y % 2) * 2 + core) * 2 + y // 2


def plane_lines(along_x):
    groups = []
    for z in range(TARGETS):
        for core in range(2):
            for at in range(4):
                if (core == 0) == along_x:
                    groups.append([device_at(z, i, at, core) for i in range(4)])
                else:
                    groups.append([device_at(z, at, i, core) for i in range(4)])
    return groups


def sent_along(value, groups):
    count = len(groups[0])
    arrived = lax.all_to_all(
        jnp.broadcast_to(value[None], (count, *value.shape)),
        AXES,
        0,
        0,
        tiled=True,
        axis_index_groups=groups,
    )
    return arrived.reshape(count * value.shape[0], *value.shape[1:])


def padded(rows):
    fill = jnp.zeros((PAD - ROWS, rows.shape[1]), rows.dtype)
    return jnp.concatenate([rows, fill], axis=0)


def row_norms(rows):
    wide = rows.astype(jnp.float32)
    return jnp.sum(wide * wide, axis=1, keepdims=True)


def prepare_kernel(at_ref, own_ref, up_ref, down_ref, far_up_ref, far_down_ref, low_ref, high_ref, t_all, norm_ref):
    half = DIM // 2

    def put(offset, piece):
        slot = lax.rem(at_ref[0] + TARGETS + offset, TARGETS)
        rows = pl.ds(pl.multiple_of(slot * PAD, PAD), PAD)
        left = padded(piece[:ROWS])
        right = padded(piece[ROWS:])
        t_all[rows, :half] = left
        t_all[rows, half:] = right
        norm_ref[rows, :] = jnp.broadcast_to(row_norms(left) + row_norms(right), (PAD, 128))

    put(0, own_ref[...])
    put(-1, up_ref[...])
    put(1, down_ref[...])
    put(-2, far_up_ref[: 2 * ROWS])
    put(-3, far_up_ref[2 * ROWS :])
    put(2, far_down_ref[: 2 * ROWS])
    put(3, far_down_ref[2 * ROWS :])
    put(4, jnp.concatenate([low_ref[...], high_ref[...]], axis=0))


def prepared(at, pieces):
    whole = TARGETS * PAD
    return pl.pallas_call(
        prepare_kernel,
        in_specs=[pl.BlockSpec(memory_space=pltpu.SMEM)]
        + [pl.BlockSpec(memory_space=pltpu.VMEM)] * len(pieces),
        out_specs=[pl.BlockSpec(memory_space=pltpu.VMEM)] * 2,
        out_shape=[
            jax.ShapeDtypeStruct((whole, DIM), jnp.bfloat16),
            jax.ShapeDtypeStruct((whole, 128), jnp.float32),
        ],
    )(at, *pieces)


def moved(value, steps):
    return lax.ppermute(value, "z", [(i, (i + steps) % TARGETS) for i in range(TARGETS)])


def half_kernel(first, spread_ref, t_hbm, norm_hbm, source_hbm, *refs):
    if first:
        out_hbm, t_all, norms, pieces, x_all, s_all, low_all, out, sems, out_sems = refs
    else:
        before_hbm, out_hbm, t_all, norms, pieces, x_all, s_all, low_all, out, before, sems, out_sems = refs
    inverse = 1.0 / spread_ref[0]
    chunks = PIECES // CHUNK
    loads = [
        pltpu.make_async_copy(
            source_hbm.at[pl.ds(j * CHUNK, CHUNK)], pieces.at[pl.ds(j * CHUNK, CHUNK)], sems.at[j]
        )
        for j in range(chunks)
    ]
    t_load = pltpu.make_async_copy(t_hbm, t_all, sems.at[chunks])
    norm_load = pltpu.make_async_copy(norm_hbm, norms, sems.at[chunks + 1])
    loads[0].start()
    t_load.start()
    norm_load.start()
    for load in loads[1:]:
        load.start()
    if not first:
        before_load = pltpu.make_async_copy(before_hbm, before, sems.at[chunks + 2])
        before_load.start()
    row_total = jnp.zeros((TARGETS * PAD, 1), jnp.float32)
    per_step = STEP // CHUNK
    for step in range(PIECES // STEP):
        for j in range(step * per_step, (step + 1) * per_step):
            loads[j].wait()
            for i in range(j * CHUNK, (j + 1) * CHUNK):
                x_all[pl.ds(i * PAD, PAD), :] = padded(pieces[i, :ROWS])
                s_all[pl.ds(i * PAD, PAD), :] = padded(pieces[i, ROWS:])
        if step == 0:
            t_load.wait()
            norm_load.wait()
        rows = pl.ds(step * STEP * PAD, STEP * PAD)
        source = x_all[rows, :]
        source_norm = row_norms(source)
        source_norm = jnp.transpose(jnp.broadcast_to(source_norm, (STEP * PAD, 128)))[:1]
        dots = lax.dot_general(
            t_all[...], source, (((1,), (1,)), ((), ())), preferred_element_type=jnp.float32
        )
        squared = jnp.maximum(norms[:, :1] + source_norm - 2.0 * dots, 0.0)
        weights = jnp.exp(-squared * inverse)
        column = lax.broadcasted_iota(jnp.int32, weights.shape, 1)
        weights = jnp.where(column % PAD < ROWS, weights, 0.0)
        low_all[:, rows] = weights.astype(jnp.bfloat16)
        row_total = row_total + jnp.sum(weights, axis=1, keepdims=True)
    if not first:
        before_load.wait()
    stores = []
    for n in range(DIM // WIDTH):
        columns = pl.ds(n * WIDTH, WIDTH)
        low = low_all[...]
        pull = jnp.dot(low, x_all[:, columns], preferred_element_type=jnp.float32)
        drive = jnp.dot(low, s_all[:, columns], preferred_element_type=jnp.float32)
        wide = t_all[:, columns].astype(jnp.float32)
        added = drive + (2.0 * inverse) * (wide * row_total - pull)
        for i in range(TARGETS):
            span = pl.ds(i * SPAN, SPAN)
            part = added[i * PAD : i * PAD + SPAN]
            if not first:
                part = (before[span, columns] + part) / POPULATION
            out[span, columns] = part
        stores.append(
            pltpu.make_async_copy(out.at[:, columns], out_hbm.at[:, columns], out_sems.at[n])
        )
        stores[-1].start()
    for store in stores:
        store.wait()


def half(spread, targets, norms, source, before=None):
    first = before is None
    whole = TARGETS * PAD
    result = (TARGETS * SPAN, DIM)
    args = [spread, targets, norms, source] + ([] if first else [before])
    scratch = [
        pltpu.VMEM((whole, DIM), jnp.bfloat16),
        pltpu.VMEM((whole, 128), jnp.float32),
        pltpu.VMEM((PIECES, 2 * ROWS, DIM), jnp.bfloat16),
        pltpu.VMEM((PIECES * PAD, DIM), jnp.bfloat16),
        pltpu.VMEM((PIECES * PAD, DIM), jnp.bfloat16),
        pltpu.VMEM((whole, PIECES * PAD), jnp.bfloat16),
        pltpu.VMEM(result, jnp.float32),
    ]
    if not first:
        scratch.append(pltpu.VMEM(result, jnp.float32))
    scratch += [
        pltpu.SemaphoreType.DMA((PIECES // CHUNK + 3,)),
        pltpu.SemaphoreType.DMA((DIM // WIDTH,)),
    ]

    def body(*refs):
        half_kernel(first, *refs)

    return pl.pallas_call(
        body,
        in_specs=[pl.BlockSpec(memory_space=pltpu.SMEM)]
        + [pl.BlockSpec(memory_space=pl.ANY)] * (len(args) - 1),
        out_specs=pl.BlockSpec(memory_space=pl.ANY),
        out_shape=jax.ShapeDtypeStruct(result, jnp.float32),
        scratch_shapes=scratch,
    )(*args)


def direction(particles, scores, spread):
    swap = [(0, 1), (1, 0)]
    at = lax.axis_index("z").astype(jnp.int32)[None]
    own_piece = jnp.concatenate([particles[:, : DIM // 2], particles[:, DIM // 2 :]], axis=0)
    up, down = moved(own_piece, 1), moved(own_piece, -1)
    far_up = moved(jnp.concatenate([own_piece, up], axis=0), 2)
    far_down = moved(jnp.concatenate([own_piece, down], axis=0), -2)
    low = moved(up[:CUT], 3)
    high = moved(down[CUT:], -3)
    targets, norms = prepared(at, [own_piece, up, down, far_up, far_down, low, high])
    line = sent_along(jnp.concatenate([particles, scores], axis=0), plane_lines(True))
    own = sent_along(line, plane_lines(False)).reshape(PIECES, 2 * ROWS, DIM)
    other = lax.ppermute(own, "c", swap)
    mine = half(spread, targets, norms, own)
    partial = half(spread, targets, norms, other, mine)
    total = lax.psum_scatter(partial, "z", scatter_dimension=0, tiled=True)
    return lax.optimization_barrier(total)[:ROWS]


def solution(mesh):
    fine = Mesh(mesh.devices.reshape(8, 4, 2, 2, 2), AXES)
    return jax.shard_map(
        direction,
        mesh=fine,
        in_specs=(P(AXES, None), P(AXES, None), P()),
        out_specs=P(AXES, None),
        check_vma=False,
    )
```

```python
import jax
import jax.numpy as jnp
from jax import lax
from jax.experimental import pallas as pl
from jax.experimental.pallas import tpu as pltpu
from jax.sharding import Mesh, PartitionSpec as P


AXES = ("z", "x", "yl", "c", "yh")
POPULATION = 7168
ROWS = 28
PAD = 32
SPAN = 31
CUT = 32
DIM = 2048
TARGETS = 8
PIECES = 16
STEP = 8
WIDTH = 512
VMEM_BYTES = 24 * 2**20


def device_at(z, x, y, core):
    return (((z * 4 + x) * 2 + y % 2) * 2 + core) * 2 + y // 2


def plane_lines(along_x):
    groups = []
    for z in range(TARGETS):
        for core in range(2):
            for at in range(4):
                if (core == 0) == along_x:
                    groups.append([device_at(z, i, at, core) for i in range(4)])
                else:
                    groups.append([device_at(z, at, i, core) for i in range(4)])
    return groups


def sent_along(value, groups):
    count = len(groups[0])
    arrived = lax.all_to_all(
        jnp.broadcast_to(value[None], (count, *value.shape)),
        AXES,
        0,
        0,
        tiled=True,
        axis_index_groups=groups,
    )
    return arrived.reshape(count * value.shape[0], *value.shape[1:])


def padded(rows):
    fill = jnp.zeros((PAD - ROWS, rows.shape[1]), rows.dtype)
    return jnp.concatenate([rows, fill], axis=0)


def row_norms(rows):
    wide = rows.astype(jnp.float32)
    return jnp.sum(wide * wide, axis=1, keepdims=True)


def prepare_kernel(at_ref, own_ref, up_ref, down_ref, far_up_ref, far_down_ref, low_ref, high_ref, t_all, norm_ref):
    half = DIM // 2

    def put(offset, piece):
        slot = lax.rem(at_ref[0] + TARGETS + offset, TARGETS)
        rows = pl.ds(pl.multiple_of(slot * PAD, PAD), PAD)
        left = padded(piece[:ROWS])
        right = padded(piece[ROWS:])
        t_all[rows, :half] = left
        t_all[rows, half:] = right
        norm_ref[rows, :] = jnp.broadcast_to(row_norms(left) + row_norms(right), (PAD, 128))

    put(0, own_ref[...])
    put(-1, up_ref[...])
    put(1, down_ref[...])
    put(-2, far_up_ref[: 2 * ROWS])
    put(-3, far_up_ref[2 * ROWS :])
    put(2, far_down_ref[: 2 * ROWS])
    put(3, far_down_ref[2 * ROWS :])
    put(4, jnp.concatenate([low_ref[...], high_ref[...]], axis=0))


def prepared(at, pieces):
    whole = TARGETS * PAD
    return pl.pallas_call(
        prepare_kernel,
        in_specs=[pl.BlockSpec(memory_space=pltpu.SMEM)]
        + [pl.BlockSpec(memory_space=pltpu.VMEM)] * len(pieces),
        out_specs=[pl.BlockSpec(memory_space=pltpu.VMEM)] * 2,
        out_shape=[
            jax.ShapeDtypeStruct((whole, DIM), jnp.bfloat16),
            jax.ShapeDtypeStruct((whole, 128), jnp.float32),
        ],
        compiler_params=pltpu.CompilerParams(vmem_limit_bytes=VMEM_BYTES),
    )(at, *pieces)


def moved(value, steps):
    return lax.ppermute(value, "z", [(i, (i + steps) % TARGETS) for i in range(TARGETS)])


def half_kernel(first, spread_ref, t_all, norms, pieces, *refs):
    if first:
        out, x_all, s_all, low_all = refs
    else:
        before, out, x_all, s_all, low_all = refs
    inverse = 1.0 / spread_ref[0]
    row_total = jnp.zeros((TARGETS * PAD, 1), jnp.float32)
    for step in range(PIECES // STEP):
        for i in range(step * STEP, (step + 1) * STEP):
            x_all[pl.ds(i * PAD, PAD), :] = padded(pieces[i, :ROWS])
            s_all[pl.ds(i * PAD, PAD), :] = padded(pieces[i, ROWS:])
        rows = pl.ds(step * STEP * PAD, STEP * PAD)
        source = x_all[rows, :]
        source_norm = row_norms(source)
        source_norm = jnp.transpose(jnp.broadcast_to(source_norm, (STEP * PAD, 128)))[:1]
        dots = lax.dot_general(
            t_all[...], source, (((1,), (1,)), ((), ())), preferred_element_type=jnp.float32
        )
        squared = jnp.maximum(norms[:, :1] + source_norm - 2.0 * dots, 0.0)
        weights = jnp.exp(-squared * inverse)
        column = lax.broadcasted_iota(jnp.int32, weights.shape, 1)
        weights = jnp.where(column % PAD < ROWS, weights, 0.0)
        low_all[:, rows] = weights.astype(jnp.bfloat16)
        row_total = row_total + jnp.sum(weights, axis=1, keepdims=True)
    for n in range(DIM // WIDTH):
        columns = pl.ds(n * WIDTH, WIDTH)
        low = low_all[...]
        pull = jnp.dot(low, x_all[:, columns], preferred_element_type=jnp.float32)
        drive = jnp.dot(low, s_all[:, columns], preferred_element_type=jnp.float32)
        wide = t_all[:, columns].astype(jnp.float32)
        added = drive + (2.0 * inverse) * (wide * row_total - pull)
        for i in range(TARGETS):
            span = pl.ds(i * SPAN, SPAN)
            part = added[i * PAD : i * PAD + SPAN]
            if not first:
                part = (before[span, columns] + part) / POPULATION
            out[span, columns] = part


def half(spread, targets, norms, source, before=None):
    first = before is None
    whole = TARGETS * PAD
    result = (TARGETS * SPAN, DIM)
    args = [targets, norms, source] + ([] if first else [before])
    args = [pltpu.with_memory_space_constraint(a, pltpu.VMEM) for a in args]

    def body(*refs):
        half_kernel(first, *refs)

    return pl.pallas_call(
        body,
        in_specs=[pl.BlockSpec(memory_space=pltpu.SMEM)]
        + [pl.BlockSpec(memory_space=pltpu.VMEM)] * len(args),
        out_specs=pl.BlockSpec(memory_space=pltpu.VMEM),
        out_shape=pltpu.VMEM(result, jnp.float32),
        scratch_shapes=[
            pltpu.VMEM((PIECES * PAD, DIM), jnp.bfloat16),
            pltpu.VMEM((PIECES * PAD, DIM), jnp.bfloat16),
            pltpu.VMEM((whole, PIECES * PAD), jnp.bfloat16),
        ],
        compiler_params=pltpu.CompilerParams(vmem_limit_bytes=VMEM_BYTES),
    )(spread, *args)


def direction(particles, scores, spread):
    swap = [(0, 1), (1, 0)]
    at = lax.axis_index("z").astype(jnp.int32)[None]
    own_piece = jnp.concatenate([particles[:, : DIM // 2], particles[:, DIM // 2 :]], axis=0)
    up, down = moved(own_piece, 1), moved(own_piece, -1)
    far_up = moved(jnp.concatenate([own_piece, up], axis=0), 2)
    far_down = moved(jnp.concatenate([own_piece, down], axis=0), -2)
    low = moved(up[:CUT], 3)
    high = moved(down[CUT:], -3)
    targets, norms = prepared(at, [own_piece, up, down, far_up, far_down, low, high])
    line = sent_along(jnp.concatenate([particles, scores], axis=0), plane_lines(True))
    own = sent_along(line, plane_lines(False)).reshape(PIECES, 2 * ROWS, DIM)
    other = lax.ppermute(own, "c", swap)
    mine = half(spread, targets, norms, own)
    partial = half(spread, targets, norms, other, mine)
    total = lax.psum_scatter(partial, "z", scatter_dimension=0, tiled=True)
    return lax.optimization_barrier(total)[:ROWS]


def solution(mesh):
    fine = Mesh(mesh.devices.reshape(8, 4, 2, 2, 2), AXES)
    return jax.shard_map(
        direction,
        mesh=fine,
        in_specs=(P(AXES, None), P(AXES, None), P()),
        out_specs=P(AXES, None),
        check_vma=False,
    )
```

```python
import jax
import jax.numpy as jnp
from jax import lax
from jax.experimental import pallas as pl
from jax.experimental.pallas import tpu as pltpu
from jax.sharding import Mesh, PartitionSpec as P


AXES = ("z", "x", "yl", "c", "yh")
POPULATION = 7168
ROWS = 28
PAD = 32
SPAN = 31
CUT = 32
DIM = 2048
TARGETS = 8
PIECES = 16
STEP = 8
WIDTH = 512
VMEM_BYTES = 24 * 2**20


def device_at(z, x, y, core):
    return (((z * 4 + x) * 2 + y % 2) * 2 + core) * 2 + y // 2


def plane_lines(along_x):
    groups = []
    for z in range(TARGETS):
        for core in range(2):
            for at in range(4):
                if (core == 0) == along_x:
                    groups.append([device_at(z, i, at, core) for i in range(4)])
                else:
                    groups.append([device_at(z, at, i, core) for i in range(4)])
    return groups


def sent_along(value, groups):
    count = len(groups[0])
    arrived = lax.all_to_all(
        jnp.broadcast_to(value[None], (count, *value.shape)),
        AXES,
        0,
        0,
        tiled=True,
        axis_index_groups=groups,
    )
    return arrived.reshape(count * value.shape[0], *value.shape[1:])


def padded(rows):
    fill = jnp.zeros((PAD - ROWS, rows.shape[1]), rows.dtype)
    return jnp.concatenate([rows, fill], axis=0)


def row_norms(rows):
    wide = rows.astype(jnp.float32)
    return jnp.sum(wide * wide, axis=1, keepdims=True)


def prepare_kernel(at_ref, own_ref, up_ref, down_ref, far_up_ref, far_down_ref, low_ref, high_ref, t_all):
    half = DIM // 2

    def put(offset, piece):
        slot = lax.rem(at_ref[0] + TARGETS + offset, TARGETS)
        rows = pl.ds(pl.multiple_of(slot * PAD, PAD), PAD)
        left = padded(piece[:ROWS])
        right = padded(piece[ROWS:])
        t_all[rows, :half] = left
        t_all[rows, half:] = right

    put(0, own_ref[...])
    put(-1, up_ref[...])
    put(1, down_ref[...])
    put(-2, far_up_ref[: 2 * ROWS])
    put(-3, far_up_ref[2 * ROWS :])
    put(2, far_down_ref[: 2 * ROWS])
    put(3, far_down_ref[2 * ROWS :])
    put(4, jnp.concatenate([low_ref[...], high_ref[...]], axis=0))


def prepared(at, pieces):
    return pl.pallas_call(
        prepare_kernel,
        in_specs=[pl.BlockSpec(memory_space=pltpu.SMEM)]
        + [pl.BlockSpec(memory_space=pltpu.VMEM)] * len(pieces),
        out_specs=pl.BlockSpec(memory_space=pltpu.VMEM),
        out_shape=pltpu.VMEM((TARGETS * PAD, DIM), jnp.bfloat16),
        compiler_params=pltpu.CompilerParams(vmem_limit_bytes=VMEM_BYTES),
    )(at, *pieces)


def moved_across(value, steps):
    pairs = [
        (group[i], group[(i + steps) % 4]) for group in plane_lines(False) for i in range(4)
    ]
    return lax.ppermute(value, AXES, sorted(pairs))


def moved(value, steps):
    return lax.ppermute(value, "z", [(i, (i + steps) % TARGETS) for i in range(TARGETS)])


def part_kernel(spread_ref, t_all, line_ref, back_ref, ahead_ref, low_ref, high_ref, out, x_all, s_all, low_all):
    inverse = 1.0 / spread_ref[0]
    targets = t_all[...]
    target_norm = row_norms(targets)
    row_total = jnp.zeros((TARGETS * PAD, 1), jnp.float32)
    pieces = [
        (ref, i * 2 * ROWS)
        for ref, count in ((line_ref, 4), (back_ref, 4), (ahead_ref, 4), (low_ref, 2), (high_ref, 2))
        for i in range(count)
    ]
    for step in range(PIECES // STEP):
        for i in range(step * STEP, (step + 1) * STEP):
            ref, at = pieces[i]
            x_all[pl.ds(i * PAD, PAD), :] = padded(ref[at : at + ROWS])
            s_all[pl.ds(i * PAD, PAD), :] = padded(ref[at + ROWS : at + 2 * ROWS])
        rows = pl.ds(step * STEP * PAD, STEP * PAD)
        source = x_all[rows, :]
        source_norm = row_norms(source)
        source_norm = jnp.transpose(jnp.broadcast_to(source_norm, (STEP * PAD, 128)))[:1]
        dots = lax.dot_general(
            targets, source, (((1,), (1,)), ((), ())), preferred_element_type=jnp.float32
        )
        squared = jnp.maximum(target_norm + source_norm - 2.0 * dots, 0.0)
        weights = jnp.exp(-squared * inverse)
        column = lax.broadcasted_iota(jnp.int32, weights.shape, 1)
        weights = jnp.where(column % PAD < ROWS, weights, 0.0)
        low_all[:, rows] = weights.astype(jnp.bfloat16)
        row_total = row_total + jnp.sum(weights, axis=1, keepdims=True)
    for n in range(DIM // WIDTH):
        columns = pl.ds(n * WIDTH, WIDTH)
        low = low_all[...]
        pull = jnp.dot(low, x_all[:, columns], preferred_element_type=jnp.float32)
        drive = jnp.dot(low, s_all[:, columns], preferred_element_type=jnp.float32)
        wide = t_all[:, columns].astype(jnp.float32)
        added = drive + (2.0 * inverse) * (wide * row_total - pull)
        for i in range(TARGETS):
            out[pl.ds(i * SPAN, SPAN), columns] = added[i * PAD : i * PAD + SPAN]


def part(spread, targets, sources):
    args = [pltpu.with_memory_space_constraint(a, pltpu.VMEM) for a in (targets, *sources)]
    return pl.pallas_call(
        part_kernel,
        in_specs=[pl.BlockSpec(memory_space=pltpu.SMEM)]
        + [pl.BlockSpec(memory_space=pltpu.VMEM)] * len(args),
        out_specs=pl.BlockSpec(memory_space=pltpu.VMEM),
        out_shape=pltpu.VMEM((TARGETS * SPAN, DIM), jnp.float32),
        scratch_shapes=[
            pltpu.VMEM((PIECES * PAD, DIM), jnp.bfloat16),
            pltpu.VMEM((PIECES * PAD, DIM), jnp.bfloat16),
            pltpu.VMEM((TARGETS * PAD, PIECES * PAD), jnp.bfloat16),
        ],
        compiler_params=pltpu.CompilerParams(vmem_limit_bytes=VMEM_BYTES),
    )(spread, *args)


def direction(particles, scores, spread):
    swap = [(0, 1), (1, 0)]
    at = lax.axis_index("z").astype(jnp.int32)[None]
    own_piece = jnp.concatenate([particles[:, : DIM // 2], particles[:, DIM // 2 :]], axis=0)
    up, down = moved(own_piece, 1), moved(own_piece, -1)
    far_up = moved(jnp.concatenate([own_piece, up], axis=0), 2)
    far_down = moved(jnp.concatenate([own_piece, down], axis=0), -2)
    low = moved(up[:CUT], 3)
    high = moved(down[CUT:], -3)
    targets = prepared(at, [own_piece, up, down, far_up, far_down, low, high])
    others = lax.ppermute(targets, "c", swap)
    line = sent_along(jnp.concatenate([particles, scores], axis=0), plane_lines(True))
    back, ahead = moved_across(line, 1), moved_across(line, -1)
    middle = 4 * ROWS
    low_half, high_half = back[:middle], ahead[middle:]
    opposite = [moved_across(low_half, 1), moved_across(high_half, -1)]
    sources = [line, back, ahead, *opposite]
    theirs = part(spread, others, sources)
    arrived = lax.ppermute(theirs, "c", swap)
    mine = part(spread, targets, sources)
    partial = (mine + arrived) / POPULATION
    total = lax.psum_scatter(partial, "z", scatter_dimension=0, tiled=True)
    return lax.optimization_barrier(total)[:ROWS]


def solution(mesh):
    fine = Mesh(mesh.devices.reshape(8, 4, 2, 2, 2), AXES)
    return jax.shard_map(
        direction,
        mesh=fine,
        in_specs=(P(AXES, None), P(AXES, None), P()),
        out_specs=P(AXES, None),
        check_vma=False,
    )
```

```python
import jax
import jax.numpy as jnp
from jax import lax
from jax.experimental import pallas as pl
from jax.experimental.pallas import tpu as pltpu
from jax.sharding import Mesh, PartitionSpec as P


AXES = ("z", "x", "yl", "c", "yh")
POPULATION = 7168
ROWS = 28
PAD = 32
SPAN = 31
CUT = 32
DIM = 2048
TARGETS = 8
PIECES = 16
STEP = 8
WIDTH = 512
VMEM_BYTES = 24 * 2**20


def device_at(z, x, y, core):
    return (((z * 4 + x) * 2 + y % 2) * 2 + core) * 2 + y // 2


def plane_lines(along_x):
    groups = []
    for z in range(TARGETS):
        for core in range(2):
            for at in range(4):
                if (core == 0) == along_x:
                    groups.append([device_at(z, i, at, core) for i in range(4)])
                else:
                    groups.append([device_at(z, at, i, core) for i in range(4)])
    return groups


def sent_along(value, groups):
    count = len(groups[0])
    arrived = lax.all_to_all(
        jnp.broadcast_to(value[None], (count, *value.shape)),
        AXES,
        0,
        0,
        tiled=True,
        axis_index_groups=groups,
    )
    return arrived.reshape(count * arrived.shape[1], *arrived.shape[2:])


def padded(rows):
    fill = jnp.zeros((PAD - ROWS, rows.shape[1]), rows.dtype)
    return jnp.concatenate([rows, fill], axis=0)


def row_norms(rows):
    wide = rows.astype(jnp.float32)
    return jnp.sum(wide * wide, axis=1, keepdims=True)


def prepare_kernel(at_ref, own_ref, up_ref, down_ref, up2_ref, down2_ref, far_up_ref, far_down_ref, t_all):
    half = DIM // 2

    def put(offset, piece):
        slot = lax.rem(at_ref[0] + TARGETS + offset, TARGETS)
        rows = pl.ds(pl.multiple_of(slot * PAD, PAD), PAD)
        left = padded(piece[:ROWS])
        right = padded(piece[ROWS:])
        t_all[rows, :half] = left
        t_all[rows, half:] = right

    put(0, own_ref[...])
    put(-1, up_ref[...])
    put(1, down_ref[...])
    put(-2, up2_ref[...])
    put(2, down2_ref[...])
    put(-3, far_up_ref[: 2 * ROWS])
    put(3, far_down_ref[: 2 * ROWS])
    put(4, jnp.concatenate([far_up_ref[2 * ROWS :], far_down_ref[2 * ROWS :]], axis=0))


def prepared(at, pieces):
    return pl.pallas_call(
        prepare_kernel,
        in_specs=[pl.BlockSpec(memory_space=pltpu.SMEM)]
        + [pl.BlockSpec(memory_space=pltpu.VMEM)] * len(pieces),
        out_specs=pl.BlockSpec(memory_space=pltpu.VMEM),
        out_shape=pltpu.VMEM((TARGETS * PAD, DIM), jnp.bfloat16),
        compiler_params=pltpu.CompilerParams(vmem_limit_bytes=VMEM_BYTES),
    )(at, *pieces)


def moved_across(value, steps):
    pairs = [
        (group[i], group[(i + steps) % 4]) for group in plane_lines(False) for i in range(4)
    ]
    return lax.ppermute(value, AXES, sorted(pairs))


def moved(value, steps):
    return lax.ppermute(value, "z", [(i, (i + steps) % TARGETS) for i in range(TARGETS)])


def part_kernel(spread_ref, t_all, line_ref, back_ref, ahead_ref, low_ref, high_ref, out, x_all, s_all, low_all):
    inverse = 1.0 / spread_ref[0]
    targets = t_all[...]
    target_norm = row_norms(targets)
    row_total = jnp.zeros((TARGETS * PAD, 1), jnp.float32)
    pieces = [
        (ref, i * 2 * ROWS)
        for ref, count in ((line_ref, 4), (back_ref, 4), (ahead_ref, 4), (low_ref, 2), (high_ref, 2))
        for i in range(count)
    ]
    for step in range(PIECES // STEP):
        for i in range(step * STEP, (step + 1) * STEP):
            ref, at = pieces[i]
            x_all[pl.ds(i * PAD, PAD), :] = padded(ref[at : at + ROWS])
            s_all[pl.ds(i * PAD, PAD), :] = padded(ref[at + ROWS : at + 2 * ROWS])
        rows = pl.ds(step * STEP * PAD, STEP * PAD)
        source = x_all[rows, :]
        source_norm = row_norms(source)
        source_norm = jnp.transpose(jnp.broadcast_to(source_norm, (STEP * PAD, 128)))[:1]
        dots = lax.dot_general(
            targets, source, (((1,), (1,)), ((), ())), preferred_element_type=jnp.float32
        )
        squared = jnp.maximum(target_norm + source_norm - 2.0 * dots, 0.0)
        weights = jnp.exp(-squared * inverse)
        column = lax.broadcasted_iota(jnp.int32, weights.shape, 1)
        weights = jnp.where(column % PAD < ROWS, weights, 0.0)
        low_all[:, rows] = weights.astype(jnp.bfloat16)
        row_total = row_total + jnp.sum(weights, axis=1, keepdims=True)
    for n in range(DIM // WIDTH):
        columns = pl.ds(n * WIDTH, WIDTH)
        low = low_all[...]
        pull = jnp.dot(low, x_all[:, columns], preferred_element_type=jnp.float32)
        drive = jnp.dot(low, s_all[:, columns], preferred_element_type=jnp.float32)
        wide = t_all[:, columns].astype(jnp.float32)
        added = drive + (2.0 * inverse) * (wide * row_total - pull)
        for i in range(TARGETS):
            out[pl.ds(i * SPAN, SPAN), columns] = added[i * PAD : i * PAD + SPAN]


def part(spread, targets, sources):
    args = [pltpu.with_memory_space_constraint(a, pltpu.VMEM) for a in (targets, *sources)]
    return pl.pallas_call(
        part_kernel,
        in_specs=[pl.BlockSpec(memory_space=pltpu.SMEM)]
        + [pl.BlockSpec(memory_space=pltpu.VMEM)] * len(args),
        out_specs=pl.BlockSpec(memory_space=pltpu.VMEM),
        out_shape=pltpu.VMEM((TARGETS * SPAN, DIM), jnp.float32),
        scratch_shapes=[
            pltpu.VMEM((PIECES * PAD, DIM), jnp.bfloat16),
            pltpu.VMEM((PIECES * PAD, DIM), jnp.bfloat16),
            pltpu.VMEM((TARGETS * PAD, PIECES * PAD), jnp.bfloat16),
        ],
        compiler_params=pltpu.CompilerParams(vmem_limit_bytes=VMEM_BYTES),
    )(spread, *args)


def direction(particles, scores, spread):
    swap = [(0, 1), (1, 0)]
    at = lax.axis_index("z").astype(jnp.int32)[None]
    own_piece = jnp.concatenate([particles[:, : DIM // 2], particles[:, DIM // 2 :]], axis=0)
    up, down = moved(own_piece, 1), moved(own_piece, -1)
    up2, down2 = moved(up, 1), moved(down, -1)
    far_up = moved(jnp.concatenate([up, up2[:CUT]], axis=0), 2)
    far_down = moved(jnp.concatenate([down, down2[CUT:]], axis=0), -2)
    targets = prepared(at, [own_piece, up, down, up2, down2, far_up, far_down])
    others = lax.ppermute(targets, "c", swap)
    line = sent_along(jnp.concatenate([particles, scores], axis=0), plane_lines(True))
    back, ahead = moved_across(line, 1), moved_across(line, -1)
    middle = 4 * ROWS
    low_half, high_half = back[:middle], ahead[middle:]
    opposite = [moved_across(low_half, 1), moved_across(high_half, -1)]
    sources = [line, back, ahead, *opposite]
    theirs = part(spread, others, sources)
    arrived = lax.ppermute(theirs, "c", swap)
    mine = part(spread, targets, sources)
    partial = (mine + arrived) / POPULATION
    total = lax.psum_scatter(partial, "z", scatter_dimension=0, tiled=True)
    return lax.optimization_barrier(total)[:ROWS]


def solution(mesh):
    fine = Mesh(mesh.devices.reshape(8, 4, 2, 2, 2), AXES)
    return jax.shard_map(
        direction,
        mesh=fine,
        in_specs=(P(AXES, None), P(AXES, None), P()),
        out_specs=P(AXES, None),
        check_vma=False,
    )
```

```python
import jax
import jax.numpy as jnp
from jax import lax
from jax.experimental import pallas as pl
from jax.experimental.pallas import tpu as pltpu
from jax.sharding import Mesh, PartitionSpec as P


AXES = ("z", "x", "yl", "c", "yh")
POPULATION = 7168
ROWS = 28
PAD = 32
SPAN = 31
CUT = 32
DIM = 2048
TARGETS = 8
PIECES = 16
STEP = 8
WIDTH = 512
VMEM_BYTES = 24 * 2**20


def device_at(z, x, y, core):
    return (((z * 4 + x) * 2 + y % 2) * 2 + core) * 2 + y // 2


def plane_lines(along_x):
    groups = []
    for z in range(TARGETS):
        for core in range(2):
            for at in range(4):
                if (core == 0) == along_x:
                    groups.append([device_at(z, i, at, core) for i in range(4)])
                else:
                    groups.append([device_at(z, at, i, core) for i in range(4)])
    return groups


def sent_along(value, groups):
    count = len(groups[0])
    arrived = lax.all_to_all(
        jnp.broadcast_to(value[None], (count, *value.shape)),
        AXES,
        0,
        0,
        tiled=True,
        axis_index_groups=groups,
    )
    return arrived.reshape(count * arrived.shape[1], *arrived.shape[2:])


def padded(rows):
    fill = jnp.zeros((PAD - ROWS, rows.shape[1]), rows.dtype)
    return jnp.concatenate([rows, fill], axis=0)


def row_norms(rows):
    wide = rows.astype(jnp.float32)
    return jnp.sum(wide * wide, axis=1, keepdims=True)


def prepare_kernel(at_ref, own_ref, up_ref, down_ref, up2_ref, down2_ref, far_up_ref, far_down_ref, t_all):
    half = DIM // 2

    def put(offset, piece):
        slot = lax.rem(at_ref[0] + TARGETS + offset, TARGETS)
        rows = pl.ds(pl.multiple_of(slot * PAD, PAD), PAD)
        left = padded(piece[:ROWS])
        right = padded(piece[ROWS:])
        t_all[rows, :half] = left
        t_all[rows, half:] = right

    put(0, own_ref[...])
    put(-1, up_ref[...])
    put(1, down_ref[...])
    put(-2, up2_ref[...])
    put(2, down2_ref[...])
    put(-3, far_up_ref[: 2 * ROWS])
    put(3, far_down_ref[: 2 * ROWS])
    put(4, jnp.concatenate([far_up_ref[2 * ROWS :], far_down_ref[2 * ROWS :]], axis=0))


def prepared(at, pieces):
    return pl.pallas_call(
        prepare_kernel,
        in_specs=[pl.BlockSpec(memory_space=pltpu.SMEM)]
        + [pl.BlockSpec(memory_space=pltpu.VMEM)] * len(pieces),
        out_specs=pl.BlockSpec(memory_space=pltpu.VMEM),
        out_shape=pltpu.VMEM((TARGETS * PAD, DIM), jnp.bfloat16),
        compiler_params=pltpu.CompilerParams(vmem_limit_bytes=VMEM_BYTES),
    )(at, *pieces)


def moved_across(value, steps):
    pairs = [
        (group[i], group[(i + steps) % 4]) for group in plane_lines(False) for i in range(4)
    ]
    return lax.ppermute(value, AXES, sorted(pairs))


def moved(value, steps):
    return lax.ppermute(value, "z", [(i, (i + steps) % TARGETS) for i in range(TARGETS)])


def part_kernel(spread_ref, t_all, line_ref, *refs):
    half_refs, (out, x_all, s_all, low_all) = refs[:6], refs[6:]
    inverse = 1.0 / spread_ref[0]
    targets = t_all[...]
    target_norm = row_norms(targets)
    row_total = jnp.zeros((TARGETS * PAD, 1), jnp.float32)
    pieces = [
        (ref, i * 2 * ROWS)
        for ref, count in ((line_ref, 4), *((half, 2) for half in half_refs))
        for i in range(count)
    ]
    for step in range(PIECES // STEP):
        for i in range(step * STEP, (step + 1) * STEP):
            ref, at = pieces[i]
            x_all[pl.ds(i * PAD, PAD), :] = padded(ref[at : at + ROWS])
            s_all[pl.ds(i * PAD, PAD), :] = padded(ref[at + ROWS : at + 2 * ROWS])
        rows = pl.ds(step * STEP * PAD, STEP * PAD)
        source = x_all[rows, :]
        source_norm = row_norms(source)
        source_norm = jnp.transpose(jnp.broadcast_to(source_norm, (STEP * PAD, 128)))[:1]
        dots = lax.dot_general(
            targets, source, (((1,), (1,)), ((), ())), preferred_element_type=jnp.float32
        )
        squared = jnp.maximum(target_norm + source_norm - 2.0 * dots, 0.0)
        weights = jnp.exp(-squared * inverse)
        column = lax.broadcasted_iota(jnp.int32, weights.shape, 1)
        weights = jnp.where(column % PAD < ROWS, weights, 0.0)
        low_all[:, rows] = weights.astype(jnp.bfloat16)
        row_total = row_total + jnp.sum(weights, axis=1, keepdims=True)
    for n in range(DIM // WIDTH):
        columns = pl.ds(n * WIDTH, WIDTH)
        low = low_all[...]
        pull = jnp.dot(low, x_all[:, columns], preferred_element_type=jnp.float32)
        drive = jnp.dot(low, s_all[:, columns], preferred_element_type=jnp.float32)
        wide = t_all[:, columns].astype(jnp.float32)
        added = drive + (2.0 * inverse) * (wide * row_total - pull)
        for i in range(TARGETS):
            out[pl.ds(i * SPAN, SPAN), columns] = added[i * PAD : i * PAD + SPAN]


def part(spread, targets, sources):
    args = [pltpu.with_memory_space_constraint(a, pltpu.VMEM) for a in (targets, *sources)]
    return pl.pallas_call(
        part_kernel,
        in_specs=[pl.BlockSpec(memory_space=pltpu.SMEM)]
        + [pl.BlockSpec(memory_space=pltpu.VMEM)] * len(args),
        out_specs=pl.BlockSpec(memory_space=pltpu.VMEM),
        out_shape=pltpu.VMEM((TARGETS * SPAN, DIM), jnp.float32),
        scratch_shapes=[
            pltpu.VMEM((PIECES * PAD, DIM), jnp.bfloat16),
            pltpu.VMEM((PIECES * PAD, DIM), jnp.bfloat16),
            pltpu.VMEM((TARGETS * PAD, PIECES * PAD), jnp.bfloat16),
        ],
        compiler_params=pltpu.CompilerParams(vmem_limit_bytes=VMEM_BYTES),
    )(spread, *args)


def direction(particles, scores, spread):
    swap = [(0, 1), (1, 0)]
    at = lax.axis_index("z").astype(jnp.int32)[None]
    own_piece = jnp.concatenate([particles[:, : DIM // 2], particles[:, DIM // 2 :]], axis=0)
    up, down = moved(own_piece, 1), moved(own_piece, -1)
    up2, down2 = moved(up, 1), moved(down, -1)
    far_up = moved(jnp.concatenate([up, up2[:CUT]], axis=0), 2)
    far_down = moved(jnp.concatenate([down, down2[CUT:]], axis=0), -2)
    targets = prepared(at, [own_piece, up, down, up2, down2, far_up, far_down])
    others = lax.ppermute(targets, "c", swap)
    line = sent_along(jnp.concatenate([particles, scores], axis=0), plane_lines(True))
    middle = 4 * ROWS
    back_low = moved_across(line[:middle], 1)
    ahead_high = moved_across(line[middle:], -1)
    back_high = moved_across(line[middle:], 1)
    ahead_low = moved_across(line[:middle], -1)
    opposite = [moved_across(back_low, 1), moved_across(ahead_high, -1)]
    sources = [line, back_low, back_high, ahead_low, ahead_high, *opposite]
    theirs = part(spread, others, sources)
    arrived = lax.ppermute(theirs, "c", swap)
    mine = part(spread, targets, sources)
    partial = (mine + arrived) / POPULATION
    total = lax.psum_scatter(partial, "z", scatter_dimension=0, tiled=True)
    return lax.optimization_barrier(total)[:ROWS]


def solution(mesh):
    fine = Mesh(mesh.devices.reshape(8, 4, 2, 2, 2), AXES)
    return jax.shard_map(
        direction,
        mesh=fine,
        in_specs=(P(AXES, None), P(AXES, None), P()),
        out_specs=P(AXES, None),
        check_vma=False,
    )
```

```python
import jax
import jax.numpy as jnp
from jax import lax
from jax.experimental import pallas as pl
from jax.experimental.pallas import tpu as pltpu
from jax.sharding import Mesh, PartitionSpec as P


AXES = ("z", "x", "yl", "c", "yh")
POPULATION = 7168
ROWS = 28
PAD = 32
CUT = 32
DIM = 2048
TARGETS = 8
PIECES = 16
STEP = 8
WIDTH = 512
VMEM_BYTES = 24 * 2**20


def device_at(z, x, y, core):
    return (((z * 4 + x) * 2 + y % 2) * 2 + core) * 2 + y // 2


def plane_lines(along_x):
    groups = []
    for z in range(TARGETS):
        for core in range(2):
            for at in range(4):
                if (core == 0) == along_x:
                    groups.append([device_at(z, i, at, core) for i in range(4)])
                else:
                    groups.append([device_at(z, at, i, core) for i in range(4)])
    return groups


def sent_along(value, groups):
    count = len(groups[0])
    arrived = lax.all_to_all(
        jnp.broadcast_to(value[None], (count, *value.shape)),
        AXES,
        0,
        0,
        tiled=True,
        axis_index_groups=groups,
    )
    return arrived.reshape(count * arrived.shape[1], *arrived.shape[2:])


def padded(rows):
    fill = jnp.zeros((PAD - ROWS, rows.shape[1]), rows.dtype)
    return jnp.concatenate([rows, fill], axis=0)


def row_norms(rows):
    wide = rows.astype(jnp.float32)
    return jnp.sum(wide * wide, axis=1, keepdims=True)


def prepare_kernel(own_ref, up_ref, down_ref, up2_ref, down2_ref, far_up_ref, far_down_ref, t_all):
    half = DIM // 2

    def put(offset, piece):
        rows = pl.ds(offset % TARGETS * PAD, PAD)
        left = padded(piece[:ROWS])
        right = padded(piece[ROWS:])
        t_all[rows, :half] = left
        t_all[rows, half:] = right

    put(0, own_ref[...])
    put(-1, up_ref[...])
    put(1, down_ref[...])
    put(-2, up2_ref[...])
    put(2, down2_ref[...])
    put(-3, far_up_ref[: 2 * ROWS])
    put(3, far_down_ref[: 2 * ROWS])
    put(4, jnp.concatenate([far_up_ref[2 * ROWS :], far_down_ref[2 * ROWS :]], axis=0))


def prepared(pieces):
    return pl.pallas_call(
        prepare_kernel,
        in_specs=[pl.BlockSpec(memory_space=pltpu.VMEM)] * len(pieces),
        out_specs=pl.BlockSpec(memory_space=pltpu.VMEM),
        out_shape=pltpu.VMEM((TARGETS * PAD, DIM), jnp.bfloat16),
        compiler_params=pltpu.CompilerParams(vmem_limit_bytes=VMEM_BYTES),
    )(*pieces)


def moved_across(value, steps):
    pairs = [
        (group[i], group[(i + steps) % 4]) for group in plane_lines(False) for i in range(4)
    ]
    return lax.ppermute(value, AXES, sorted(pairs))


def moved(value, steps):
    return lax.ppermute(value, "z", [(i, (i + steps) % TARGETS) for i in range(TARGETS)])


def part_kernel(spread_ref, t_all, line_ref, *refs):
    half_refs, outs, (x_all, s_all, low_all) = refs[:6], refs[6:8], refs[8:]
    inverse = 1.0 / spread_ref[0]
    targets = t_all[...]
    target_norm = row_norms(targets)
    row_total = jnp.zeros((TARGETS * PAD, 1), jnp.float32)
    pieces = [
        (ref, i * 2 * ROWS)
        for ref, count in ((line_ref, 4), *((half, 2) for half in half_refs))
        for i in range(count)
    ]
    for step in range(PIECES // STEP):
        for i in range(step * STEP, (step + 1) * STEP):
            ref, at = pieces[i]
            x_all[pl.ds(i * PAD, PAD), :] = padded(ref[at : at + ROWS])
            s_all[pl.ds(i * PAD, PAD), :] = padded(ref[at + ROWS : at + 2 * ROWS])
        rows = pl.ds(step * STEP * PAD, STEP * PAD)
        source = x_all[rows, :]
        source_norm = row_norms(source)
        source_norm = jnp.transpose(jnp.broadcast_to(source_norm, (STEP * PAD, 128)))[:1]
        dots = lax.dot_general(
            targets, source, (((1,), (1,)), ((), ())), preferred_element_type=jnp.float32
        )
        squared = jnp.maximum(target_norm + source_norm - 2.0 * dots, 0.0)
        weights = jnp.exp(-squared * inverse)
        column = lax.broadcasted_iota(jnp.int32, weights.shape, 1)
        weights = jnp.where(column % PAD < ROWS, weights, 0.0)
        low_all[:, rows] = weights.astype(jnp.bfloat16)
        row_total = row_total + jnp.sum(weights, axis=1, keepdims=True)
    for n in range(DIM // WIDTH):
        columns = pl.ds(n * WIDTH, WIDTH)
        low = low_all[...]
        pull = jnp.dot(low, x_all[:, columns], preferred_element_type=jnp.float32)
        drive = jnp.dot(low, s_all[:, columns], preferred_element_type=jnp.float32)
        wide = t_all[:, columns].astype(jnp.float32)
        added = drive + (2.0 * inverse) * (wide * row_total - pull)
        for i in range(TARGETS):
            rows = pl.ds((2 * i + n % 2) * ROWS, ROWS)
            outs[n // 2][rows, :] = added[i * PAD : i * PAD + ROWS]


def part(spread, targets, sources):
    args = [pltpu.with_memory_space_constraint(a, pltpu.VMEM) for a in (targets, *sources)]
    return pl.pallas_call(
        part_kernel,
        in_specs=[pl.BlockSpec(memory_space=pltpu.SMEM)]
        + [pl.BlockSpec(memory_space=pltpu.VMEM)] * len(args),
        out_specs=[pl.BlockSpec(memory_space=pltpu.VMEM)] * 2,
        out_shape=[pltpu.VMEM((2 * TARGETS * ROWS, WIDTH), jnp.float32)] * 2,
        scratch_shapes=[
            pltpu.VMEM((PIECES * PAD, DIM), jnp.bfloat16),
            pltpu.VMEM((PIECES * PAD, DIM), jnp.bfloat16),
            pltpu.VMEM((TARGETS * PAD, PIECES * PAD), jnp.bfloat16),
        ],
        compiler_params=pltpu.CompilerParams(vmem_limit_bytes=VMEM_BYTES),
    )(spread, *args)


def direction(particles, scores, spread):
    swap = [(0, 1), (1, 0)]
    own_piece = jnp.concatenate([particles[:, : DIM // 2], particles[:, DIM // 2 :]], axis=0)
    up, down = moved(own_piece, 1), moved(own_piece, -1)
    up2, down2 = moved(up, 1), moved(down, -1)
    far_up = moved(jnp.concatenate([up, up2[:CUT]], axis=0), 2)
    far_down = moved(jnp.concatenate([down, down2[CUT:]], axis=0), -2)
    targets = prepared([own_piece, up, down, up2, down2, far_up, far_down])
    others = lax.ppermute(targets, "c", swap)
    line = sent_along(jnp.concatenate([particles, scores], axis=0), plane_lines(True))
    middle = 4 * ROWS
    back_low = moved_across(line[:middle], 1)
    ahead_high = moved_across(line[middle:], -1)
    back_high = moved_across(line[middle:], 1)
    ahead_low = moved_across(line[:middle], -1)
    opposite = [moved_across(back_low, 1), moved_across(ahead_high, -1)]
    sources = [line, back_low, back_high, ahead_low, ahead_high, *opposite]
    theirs = part(spread, others, sources)
    arrived = [lax.ppermute(t, "c", swap) for t in theirs]
    mine = part(spread, targets, sources)
    halves = [summed_along_z((m + a) / POPULATION) for m, a in zip(mine, arrived)]
    return jnp.concatenate([rows for h in halves for rows in (h[:ROWS], h[ROWS:])], axis=1)


def summed_along_z(partial):
    chunk = [partial[2 * ROWS * k : 2 * ROWS * (k + 1)] for k in range(TARGETS)]
    up = moved(chunk[4][:CUT], 1)
    down = moved(chunk[4][CUT:], -1)
    up = moved(jnp.concatenate([chunk[3][:CUT] + up, chunk[3][CUT:]], axis=0), 1)
    down = moved(jnp.concatenate([chunk[5][:CUT], chunk[5][CUT:] + down], axis=0), -1)
    up = moved(chunk[2] + up, 1)
    down = moved(chunk[6] + down, -1)
    up = moved(chunk[1] + up, 1)
    down = moved(chunk[7] + down, -1)
    return chunk[0] + up + down


def solution(mesh):
    fine = Mesh(mesh.devices.reshape(8, 4, 2, 2, 2), AXES)
    return jax.shard_map(
        direction,
        mesh=fine,
        in_specs=(P(AXES, None), P(AXES, None), P()),
        out_specs=P(AXES, None),
        check_vma=False,
    )
```

```python
import jax
import jax.numpy as jnp
from jax import lax
from jax.experimental import pallas as pl
from jax.experimental.pallas import tpu as pltpu
from jax.sharding import Mesh, PartitionSpec as P


AXES = ("z", "x", "yl", "c", "yh")
POPULATION = 7168
ROWS = 28
PAD = 32
CUT = 32
DIM = 2048
TARGETS = 8
PIECES = 16
STEP = 8
WIDTH = 512
VMEM_BYTES = 24 * 2**20


def device_at(z, x, y, core):
    return (((z * 4 + x) * 2 + y % 2) * 2 + core) * 2 + y // 2


def plane_lines(along_x):
    groups = []
    for z in range(TARGETS):
        for core in range(2):
            for at in range(4):
                if (core == 0) == along_x:
                    groups.append([device_at(z, i, at, core) for i in range(4)])
                else:
                    groups.append([device_at(z, at, i, core) for i in range(4)])
    return groups


def sent_along(value, groups):
    count = len(groups[0])
    arrived = lax.all_to_all(
        jnp.broadcast_to(value[None], (count, *value.shape)),
        AXES,
        0,
        0,
        tiled=True,
        axis_index_groups=groups,
    )
    return arrived.reshape(count * arrived.shape[1], *arrived.shape[2:])


def padded(rows):
    fill = jnp.zeros((PAD - ROWS, rows.shape[1]), rows.dtype)
    return jnp.concatenate([rows, fill], axis=0)


def row_norms(rows):
    wide = rows.astype(jnp.float32)
    return jnp.sum(wide * wide, axis=1, keepdims=True)


def prepare_kernel(own_ref, up_ref, down_ref, up2_ref, down2_ref, far_up_ref, far_down_ref, t_all):
    half = DIM // 2

    def put(offset, piece):
        rows = pl.ds(offset % TARGETS * PAD, PAD)
        left = padded(piece[:ROWS])
        right = padded(piece[ROWS:])
        t_all[rows, :half] = left
        t_all[rows, half:] = right

    put(0, own_ref[...])
    put(-1, up_ref[...])
    put(1, down_ref[...])
    put(-2, up2_ref[...])
    put(2, down2_ref[...])
    put(-3, far_up_ref[: 2 * ROWS])
    put(3, far_down_ref[: 2 * ROWS])
    put(4, jnp.concatenate([far_up_ref[2 * ROWS :], far_down_ref[2 * ROWS :]], axis=0))


def prepared(pieces):
    return pl.pallas_call(
        prepare_kernel,
        in_specs=[pl.BlockSpec(memory_space=pltpu.VMEM)] * len(pieces),
        out_specs=pl.BlockSpec(memory_space=pltpu.VMEM),
        out_shape=pltpu.VMEM((TARGETS * PAD, DIM), jnp.bfloat16),
        compiler_params=pltpu.CompilerParams(vmem_limit_bytes=VMEM_BYTES),
    )(*pieces)


def moved_across(value, steps):
    pairs = [
        (group[i], group[(i + steps) % 4]) for group in plane_lines(False) for i in range(4)
    ]
    return lax.ppermute(value, AXES, sorted(pairs))


def moved(value, steps):
    return lax.ppermute(value, "z", [(i, (i + steps) % TARGETS) for i in range(TARGETS)])


def part_kernel(spread_ref, t_all, line_ref, *refs):
    half_refs, (out, x_all, s_all, low_all) = refs[:6], refs[6:]
    inverse = 1.0 / spread_ref[0]
    targets = t_all[...]
    target_norm = row_norms(targets)
    row_total = jnp.zeros((TARGETS * PAD, 1), jnp.float32)
    pieces = [
        (ref, i * 2 * ROWS)
        for ref, count in ((line_ref, 4), *((half, 2) for half in half_refs))
        for i in range(count)
    ]
    for step in range(PIECES // STEP):
        for i in range(step * STEP, (step + 1) * STEP):
            ref, at = pieces[i]
            x_all[pl.ds(i * PAD, PAD), :] = padded(ref[at : at + ROWS])
            s_all[pl.ds(i * PAD, PAD), :] = padded(ref[at + ROWS : at + 2 * ROWS])
        rows = pl.ds(step * STEP * PAD, STEP * PAD)
        source = x_all[rows, :]
        source_norm = row_norms(source)
        source_norm = jnp.transpose(jnp.broadcast_to(source_norm, (STEP * PAD, 128)))[:1]
        dots = lax.dot_general(
            targets, source, (((1,), (1,)), ((), ())), preferred_element_type=jnp.float32
        )
        squared = jnp.maximum(target_norm + source_norm - 2.0 * dots, 0.0)
        weights = jnp.exp(-squared * inverse)
        column = lax.broadcasted_iota(jnp.int32, weights.shape, 1)
        weights = jnp.where(column % PAD < ROWS, weights, 0.0)
        low_all[:, rows] = weights.astype(jnp.bfloat16)
        row_total = row_total + jnp.sum(weights, axis=1, keepdims=True)
    for n in range(DIM // WIDTH):
        columns = pl.ds(n * WIDTH, WIDTH)
        low = low_all[...]
        pull = jnp.dot(low, x_all[:, columns], preferred_element_type=jnp.float32)
        drive = jnp.dot(low, s_all[:, columns], preferred_element_type=jnp.float32)
        wide = t_all[:, columns].astype(jnp.float32)
        added = drive + (2.0 * inverse) * (wide * row_total - pull)
        for i in range(TARGETS):
            rows = pl.ds((2 * i + n // 2) * ROWS, ROWS)
            out[rows, pl.ds(n % 2 * WIDTH, WIDTH)] = added[i * PAD : i * PAD + ROWS]


def part(spread, targets, sources):
    args = [pltpu.with_memory_space_constraint(a, pltpu.VMEM) for a in (targets, *sources)]
    return pl.pallas_call(
        part_kernel,
        in_specs=[pl.BlockSpec(memory_space=pltpu.SMEM)]
        + [pl.BlockSpec(memory_space=pltpu.VMEM)] * len(args),
        out_specs=pl.BlockSpec(memory_space=pltpu.VMEM),
        out_shape=pltpu.VMEM((2 * TARGETS * ROWS, 2 * WIDTH), jnp.float32),
        scratch_shapes=[
            pltpu.VMEM((PIECES * PAD, DIM), jnp.bfloat16),
            pltpu.VMEM((PIECES * PAD, DIM), jnp.bfloat16),
            pltpu.VMEM((TARGETS * PAD, PIECES * PAD), jnp.bfloat16),
        ],
        compiler_params=pltpu.CompilerParams(vmem_limit_bytes=VMEM_BYTES),
    )(spread, *args)


def direction(particles, scores, spread):
    swap = [(0, 1), (1, 0)]
    own_piece = jnp.concatenate([particles[:, : DIM // 2], particles[:, DIM // 2 :]], axis=0)
    up, down = moved(own_piece, 1), moved(own_piece, -1)
    up2, down2 = moved(up, 1), moved(down, -1)
    far_up = moved(jnp.concatenate([up, up2[:CUT]], axis=0), 2)
    far_down = moved(jnp.concatenate([down, down2[CUT:]], axis=0), -2)
    targets = prepared([own_piece, up, down, up2, down2, far_up, far_down])
    others = lax.ppermute(targets, "c", swap)
    line = sent_along(jnp.concatenate([particles, scores], axis=0), plane_lines(True))
    middle = 4 * ROWS
    back_low = moved_across(line[:middle], 1)
    ahead_high = moved_across(line[middle:], -1)
    back_high = moved_across(line[middle:], 1)
    ahead_low = moved_across(line[:middle], -1)
    opposite = [moved_across(back_low, 1), moved_across(ahead_high, -1)]
    sources = [line, back_low, back_high, ahead_low, ahead_high, *opposite]
    theirs = part(spread, others, sources)
    arrived = lax.ppermute(theirs, "c", swap)
    mine = part(spread, targets, sources)
    total = summed_along_z((mine + arrived) / POPULATION)
    return jnp.concatenate([total[:ROWS], total[ROWS:]], axis=1)


def summed_along_z(partial):
    chunk = [partial[2 * ROWS * k : 2 * ROWS * (k + 1)] for k in range(TARGETS)]
    up = moved(chunk[4][:CUT], 1)
    down = moved(chunk[4][CUT:], -1)
    up = moved(jnp.concatenate([chunk[3][:CUT] + up, chunk[3][CUT:]], axis=0), 1)
    down = moved(jnp.concatenate([chunk[5][:CUT], chunk[5][CUT:] + down], axis=0), -1)
    up = moved(chunk[2] + up, 1)
    down = moved(chunk[6] + down, -1)
    up = moved(chunk[1] + up, 1)
    down = moved(chunk[7] + down, -1)
    return chunk[0] + up + down


def solution(mesh):
    fine = Mesh(mesh.devices.reshape(8, 4, 2, 2, 2), AXES)
    return jax.shard_map(
        direction,
        mesh=fine,
        in_specs=(P(AXES, None), P(AXES, None), P()),
        out_specs=P(AXES, None),
        check_vma=False,
    )
```

```python
import jax
import jax.numpy as jnp
from jax import lax
from jax.experimental import pallas as pl
from jax.experimental.pallas import tpu as pltpu
from jax.sharding import Mesh, PartitionSpec as P


AXES = ("z", "x", "yl", "c", "yh")
POPULATION = 7168
ROWS = 28
PAD = 32
CUT = 32
DIM = 2048
TARGETS = 8
PIECES = 16
STEP = 8
WIDTH = 512
VMEM_BYTES = 24 * 2**20


def device_at(z, x, y, core):
    return (((z * 4 + x) * 2 + y % 2) * 2 + core) * 2 + y // 2


def plane_lines(along_x):
    groups = []
    for z in range(TARGETS):
        for core in range(2):
            for at in range(4):
                if (core == 0) == along_x:
                    groups.append([device_at(z, i, at, core) for i in range(4)])
                else:
                    groups.append([device_at(z, at, i, core) for i in range(4)])
    return groups


def sent_along(value, groups):
    count = len(groups[0])
    arrived = lax.all_to_all(
        jnp.broadcast_to(value[None], (count, *value.shape)),
        AXES,
        0,
        0,
        tiled=True,
        axis_index_groups=groups,
    )
    return arrived.reshape(count * arrived.shape[1], *arrived.shape[2:])


def padded(rows):
    fill = jnp.zeros((PAD - ROWS, rows.shape[1]), rows.dtype)
    return jnp.concatenate([rows, fill], axis=0)


def row_norms(rows):
    wide = rows.astype(jnp.float32)
    return jnp.sum(wide * wide, axis=1, keepdims=True)


def prepare_kernel(own_ref, up_ref, down_ref, up2_ref, down2_ref, far_up_ref, far_down_ref, t_all):
    half = DIM // 2

    def put(offset, piece):
        rows = pl.ds(offset % TARGETS * PAD, PAD)
        left = padded(piece[:ROWS])
        right = padded(piece[ROWS:])
        t_all[rows, :half] = left
        t_all[rows, half:] = right

    put(0, own_ref[...])
    put(-1, up_ref[...])
    put(1, down_ref[...])
    put(-2, up2_ref[...])
    put(2, down2_ref[...])
    put(-3, far_up_ref[: 2 * ROWS])
    put(3, far_down_ref[: 2 * ROWS])
    put(4, jnp.concatenate([far_up_ref[2 * ROWS :], far_down_ref[2 * ROWS :]], axis=0))


def prepared(pieces):
    return pl.pallas_call(
        prepare_kernel,
        in_specs=[pl.BlockSpec(memory_space=pltpu.VMEM)] * len(pieces),
        out_specs=pl.BlockSpec(memory_space=pltpu.VMEM),
        out_shape=pltpu.VMEM((TARGETS * PAD, DIM), jnp.bfloat16),
        compiler_params=pltpu.CompilerParams(vmem_limit_bytes=VMEM_BYTES),
    )(*pieces)


def moved_across(value, steps):
    pairs = [
        (group[i], group[(i + steps) % 4]) for group in plane_lines(False) for i in range(4)
    ]
    return lax.ppermute(value, AXES, sorted(pairs))


def moved(value, steps):
    return lax.ppermute(value, "z", [(i, (i + steps) % TARGETS) for i in range(TARGETS)])


def part_kernel(spread_ref, t_all, line_ref, *refs):
    half_refs, (out, x_all, s_all, low_all) = refs[:6], refs[6:]
    inverse = 1.0 / spread_ref[0]
    targets = t_all[...]
    target_norm = row_norms(targets)
    row_total = jnp.zeros((TARGETS * PAD, 1), jnp.float32)
    pieces = [
        (ref, i * 2 * ROWS)
        for ref, count in ((line_ref, 4), *((half, 2) for half in half_refs))
        for i in range(count)
    ]
    for step in range(PIECES // STEP):
        for i in range(step * STEP, (step + 1) * STEP):
            ref, at = pieces[i]
            x_all[pl.ds(i * PAD, PAD), :] = padded(ref[at : at + ROWS])
            s_all[pl.ds(i * PAD, PAD), :] = padded(ref[at + ROWS : at + 2 * ROWS])
        rows = pl.ds(step * STEP * PAD, STEP * PAD)
        source = x_all[rows, :]
        source_norm = row_norms(source)
        source_norm = jnp.transpose(jnp.broadcast_to(source_norm, (STEP * PAD, 128)))[:1]
        dots = lax.dot_general(
            targets, source, (((1,), (1,)), ((), ())), preferred_element_type=jnp.float32
        )
        squared = jnp.maximum(target_norm + source_norm - 2.0 * dots, 0.0)
        weights = jnp.exp(-squared * inverse)
        column = lax.broadcasted_iota(jnp.int32, weights.shape, 1)
        weights = jnp.where(column % PAD < ROWS, weights, 0.0)
        low_all[:, rows] = weights.astype(jnp.bfloat16)
        row_total = row_total + jnp.sum(weights, axis=1, keepdims=True)
    for n in range(DIM // WIDTH):
        columns = pl.ds(n * WIDTH, WIDTH)
        low = low_all[...]
        pull = jnp.dot(low, x_all[:, columns], preferred_element_type=jnp.float32)
        drive = jnp.dot(low, s_all[:, columns], preferred_element_type=jnp.float32)
        wide = t_all[:, columns].astype(jnp.float32)
        added = drive + (2.0 * inverse) * (wide * row_total - pull)
        for i in range(TARGETS):
            rows = pl.ds((2 * i + n // 2) * ROWS, ROWS)
            out[rows, pl.ds(n % 2 * WIDTH, WIDTH)] = added[i * PAD : i * PAD + ROWS]


def part(spread, targets, sources):
    args = [pltpu.with_memory_space_constraint(a, pltpu.VMEM) for a in (targets, *sources)]
    return pl.pallas_call(
        part_kernel,
        in_specs=[pl.BlockSpec(memory_space=pltpu.SMEM)]
        + [pl.BlockSpec(memory_space=pltpu.VMEM)] * len(args),
        out_specs=pl.BlockSpec(memory_space=pltpu.VMEM),
        out_shape=pltpu.VMEM((2 * TARGETS * ROWS, 2 * WIDTH), jnp.float32),
        scratch_shapes=[
            pltpu.VMEM((PIECES * PAD, DIM), jnp.bfloat16),
            pltpu.VMEM((PIECES * PAD, DIM), jnp.bfloat16),
            pltpu.VMEM((TARGETS * PAD, PIECES * PAD), jnp.bfloat16),
        ],
        compiler_params=pltpu.CompilerParams(vmem_limit_bytes=VMEM_BYTES),
    )(spread, *args)


def direction(particles, scores, spread):
    swap = [(0, 1), (1, 0)]
    own_piece = jnp.concatenate([particles[:, : DIM // 2], particles[:, DIM // 2 :]], axis=0)
    up, down = moved(own_piece, 1), moved(own_piece, -1)
    up2, down2 = moved(up, 1), moved(down, -1)
    far_up = moved(jnp.concatenate([up, up2[:CUT]], axis=0), 2)
    far_down = moved(jnp.concatenate([down, down2[CUT:]], axis=0), -2)
    targets = prepared([own_piece, up, down, up2, down2, far_up, far_down])
    others = lax.ppermute(targets, "c", swap)
    line = sent_along(jnp.concatenate([particles, scores], axis=0), plane_lines(True))
    middle = 4 * ROWS
    back_low = moved_across(line[:middle], 1)
    ahead_high = moved_across(line[middle:], -1)
    back_high = moved_across(line[middle:], 1)
    ahead_low = moved_across(line[:middle], -1)
    opposite = [moved_across(back_low, 1), moved_across(ahead_high, -1)]
    sources = [line, back_low, back_high, ahead_low, ahead_high, *opposite]
    theirs = part(spread, others, sources)
    arrived = lax.ppermute(theirs, "c", swap)
    mine = part(spread, targets, sources)
    total = summed_along_z(mine, arrived)
    return jnp.concatenate([total[:ROWS], total[ROWS:]], axis=1)


def summed_along_z(mine, arrived):
    size = 2 * ROWS

    def both(first, last):
        span = slice(first * size, last * size)
        return (mine[span] + arrived[span]) / POPULATION

    ahead, behind = lax.optimization_barrier((both(1, 5), both(4, 8)))

    def rows(array, index, first=0, last=size):
        return array[index * size + first : index * size + last]

    up = moved(rows(ahead, 3, 0, CUT), 1)
    down = moved(rows(behind, 0, CUT), -1)
    up = jnp.concatenate([rows(ahead, 2, 0, CUT) + up, rows(ahead, 2, CUT)], axis=0)
    down = jnp.concatenate([rows(behind, 1, 0, CUT), rows(behind, 1, CUT) + down], axis=0)
    up, down = moved(up, 1), moved(down, -1)
    up, down = moved(rows(ahead, 1) + up, 1), moved(rows(behind, 2) + down, -1)
    up, down = moved(rows(ahead, 0) + up, 1), moved(rows(behind, 3) + down, -1)
    return both(0, 1) + up + down


def solution(mesh):
    fine = Mesh(mesh.devices.reshape(8, 4, 2, 2, 2), AXES)
    return jax.shard_map(
        direction,
        mesh=fine,
        in_specs=(P(AXES, None), P(AXES, None), P()),
        out_specs=P(AXES, None),
        check_vma=False,
    )
```

```python
import jax
import jax.numpy as jnp
from jax import lax
from jax.experimental import pallas as pl
from jax.experimental.pallas import tpu as pltpu
from jax.sharding import Mesh, PartitionSpec as P


AXES = ("z", "x", "yl", "c", "yh")
POPULATION = 7168
ROWS = 28
PAD = 32
CUT = 32
DIM = 2048
TARGETS = 8
PIECES = 16
STEP = 16
WIDTH = 512
VMEM_BYTES = 24 * 2**20


def device_at(z, x, y, core):
    return (((z * 4 + x) * 2 + y % 2) * 2 + core) * 2 + y // 2


def plane_lines(along_x):
    groups = []
    for z in range(TARGETS):
        for core in range(2):
            for at in range(4):
                if (core == 0) == along_x:
                    groups.append([device_at(z, i, at, core) for i in range(4)])
                else:
                    groups.append([device_at(z, at, i, core) for i in range(4)])
    return groups


def sent_along(value, groups):
    count = len(groups[0])
    arrived = lax.all_to_all(
        jnp.broadcast_to(value[None], (count, *value.shape)),
        AXES,
        0,
        0,
        tiled=True,
        axis_index_groups=groups,
    )
    return arrived.reshape(count * arrived.shape[1], *arrived.shape[2:])


def padded(rows):
    fill = jnp.zeros((PAD - ROWS, rows.shape[1]), rows.dtype)
    return jnp.concatenate([rows, fill], axis=0)


def row_norms(rows):
    wide = rows.astype(jnp.float32)
    return jnp.sum(wide * wide, axis=1, keepdims=True)


def prepare_kernel(own_ref, up_ref, down_ref, up2_ref, down2_ref, far_up_ref, far_down_ref, t_all):
    half = DIM // 2

    def put(offset, piece):
        rows = pl.ds(offset % TARGETS * PAD, PAD)
        left = padded(piece[:ROWS])
        right = padded(piece[ROWS:])
        t_all[rows, :half] = left
        t_all[rows, half:] = right

    put(0, own_ref[...])
    put(-1, up_ref[...])
    put(1, down_ref[...])
    put(-2, up2_ref[...])
    put(2, down2_ref[...])
    put(-3, far_up_ref[: 2 * ROWS])
    put(3, far_down_ref[: 2 * ROWS])
    put(4, jnp.concatenate([far_up_ref[2 * ROWS :], far_down_ref[2 * ROWS :]], axis=0))


def prepared(pieces):
    return pl.pallas_call(
        prepare_kernel,
        in_specs=[pl.BlockSpec(memory_space=pltpu.VMEM)] * len(pieces),
        out_specs=pl.BlockSpec(memory_space=pltpu.VMEM),
        out_shape=pltpu.VMEM((TARGETS * PAD, DIM), jnp.bfloat16),
        compiler_params=pltpu.CompilerParams(vmem_limit_bytes=VMEM_BYTES),
    )(*pieces)


def moved_across(value, steps):
    pairs = [
        (group[i], group[(i + steps) % 4]) for group in plane_lines(False) for i in range(4)
    ]
    return lax.ppermute(value, AXES, sorted(pairs))


def moved(value, steps):
    return lax.ppermute(value, "z", [(i, (i + steps) % TARGETS) for i in range(TARGETS)])


def part_kernel(spread_ref, t_all, line_ref, *refs):
    half_refs, outs, (x_all, s_all, low_all) = refs[:6], refs[6:8], refs[8:]
    inverse = 1.0 / spread_ref[0]
    targets = t_all[...]
    target_norm = row_norms(targets)
    row_total = jnp.zeros((TARGETS * PAD, 1), jnp.float32)
    pieces = [
        (ref, i * 2 * ROWS)
        for ref, count in ((line_ref, 4), *((half, 2) for half in half_refs))
        for i in range(count)
    ]
    for step in range(PIECES // STEP):
        for i in range(step * STEP, (step + 1) * STEP):
            ref, at = pieces[i]
            x_all[pl.ds(i * PAD, PAD), :] = padded(ref[at : at + ROWS])
            s_all[pl.ds(i * PAD, PAD), :] = padded(ref[at + ROWS : at + 2 * ROWS])
        rows = pl.ds(step * STEP * PAD, STEP * PAD)
        source = x_all[rows, :]
        source_norm = row_norms(source)
        source_norm = jnp.transpose(jnp.broadcast_to(source_norm, (STEP * PAD, 128)))[:1]
        dots = lax.dot_general(
            targets, source, (((1,), (1,)), ((), ())), preferred_element_type=jnp.float32
        )
        squared = jnp.maximum(target_norm + source_norm - 2.0 * dots, 0.0)
        weights = jnp.exp(-squared * inverse)
        column = lax.broadcasted_iota(jnp.int32, weights.shape, 1)
        weights = jnp.where(column % PAD < ROWS, weights, 0.0)
        low_all[:, rows] = weights.astype(jnp.bfloat16)
        row_total = row_total + jnp.sum(weights, axis=1, keepdims=True)
    for n in range(DIM // WIDTH):
        columns = pl.ds(n * WIDTH, WIDTH)
        low = low_all[...]
        pull = jnp.dot(low, x_all[:, columns], preferred_element_type=jnp.float32)
        drive = jnp.dot(low, s_all[:, columns], preferred_element_type=jnp.float32)
        wide = t_all[:, columns].astype(jnp.float32)
        added = drive + (2.0 * inverse) * (wide * row_total - pull)
        for i in range(TARGETS):
            rows = pl.ds((2 * (i % 4) + n // 2) * ROWS, ROWS)
            outs[i // 4][rows, pl.ds(n % 2 * WIDTH, WIDTH)] = added[i * PAD : i * PAD + ROWS]


def part(spread, targets, sources):
    args = [pltpu.with_memory_space_constraint(a, pltpu.VMEM) for a in (targets, *sources)]
    return pl.pallas_call(
        part_kernel,
        in_specs=[pl.BlockSpec(memory_space=pltpu.SMEM)]
        + [pl.BlockSpec(memory_space=pltpu.VMEM)] * len(args),
        out_specs=[pl.BlockSpec(memory_space=pltpu.VMEM)] * 2,
        out_shape=[pltpu.VMEM((TARGETS * ROWS, 2 * WIDTH), jnp.float32)] * 2,
        scratch_shapes=[
            pltpu.VMEM((PIECES * PAD, DIM), jnp.bfloat16),
            pltpu.VMEM((PIECES * PAD, DIM), jnp.bfloat16),
            pltpu.VMEM((TARGETS * PAD, PIECES * PAD), jnp.bfloat16),
        ],
        compiler_params=pltpu.CompilerParams(vmem_limit_bytes=VMEM_BYTES),
    )(spread, *args)


def direction(particles, scores, spread):
    swap = [(0, 1), (1, 0)]
    own_piece = jnp.concatenate([particles[:, : DIM // 2], particles[:, DIM // 2 :]], axis=0)
    up, down = moved(own_piece, 1), moved(own_piece, -1)
    up2, down2 = moved(up, 1), moved(down, -1)
    far_up = moved(jnp.concatenate([up, up2[:CUT]], axis=0), 2)
    far_down = moved(jnp.concatenate([down, down2[CUT:]], axis=0), -2)
    targets = prepared([own_piece, up, down, up2, down2, far_up, far_down])
    others = lax.ppermute(targets, "c", swap)
    line = sent_along(jnp.concatenate([particles, scores], axis=0), plane_lines(True))
    middle = 4 * ROWS
    back_low = moved_across(line[:middle], 1)
    ahead_high = moved_across(line[middle:], -1)
    back_high = moved_across(line[middle:], 1)
    ahead_low = moved_across(line[:middle], -1)
    opposite = [moved_across(back_low, 1), moved_across(ahead_high, -1)]
    sources = [line, back_low, back_high, ahead_low, ahead_high, *opposite]
    theirs = part(spread, others, sources)
    arrived_behind = lax.ppermute(theirs[1], "c", swap)
    arrived_ahead = lax.ppermute(theirs[0], "c", swap)
    mine = part(spread, targets, sources)
    behind = lax.optimization_barrier((mine[1] + arrived_behind) / POPULATION)
    ahead = lax.optimization_barrier((mine[0] + arrived_ahead) / POPULATION)
    total = summed_along_z(ahead, behind)
    return jnp.concatenate([total[:ROWS], total[ROWS:]], axis=1)


def summed_along_z(ahead, behind):
    size = 2 * ROWS

    def rows(array, index, first=0, last=size):
        return array[index * size + first : index * size + last]

    up = moved(rows(behind, 0, 0, CUT), 1)
    down = moved(rows(behind, 0, CUT), -1)
    up = jnp.concatenate([rows(ahead, 3, 0, CUT) + up, rows(ahead, 3, CUT)], axis=0)
    down = jnp.concatenate([rows(behind, 1, 0, CUT), rows(behind, 1, CUT) + down], axis=0)
    up, down = moved(up, 1), moved(down, -1)
    up, down = moved(rows(ahead, 2) + up, 1), moved(rows(behind, 2) + down, -1)
    up, down = moved(rows(ahead, 1) + up, 1), moved(rows(behind, 3) + down, -1)
    return rows(ahead, 0) + up + down


def solution(mesh):
    fine = Mesh(mesh.devices.reshape(8, 4, 2, 2, 2), AXES)
    return jax.shard_map(
        direction,
        mesh=fine,
        in_specs=(P(AXES, None), P(AXES, None), P()),
        out_specs=P(AXES, None),
        check_vma=False,
    )
```
